32 devices in a mesh: rep: 1 (over z), dp: 32 (over x, y, core).
Axes of the slice: x: 4, y: 4, z: 1, core: 2. Of those that a mesh axis runs over, the one named last changes fastest.
The devices are a block of a 4x4x8 slice.
Arguments:
- x: bfloat16 [32, 2048, 896], P(('rep', 'dp'))
- dy: bfloat16 [32, 2048, 896], P(('rep', 'dp'))
- wq: bfloat16 [2, 896, 896], P(None, 'dp')
- wk: bfloat16 [2, 896, 896], P(None, 'dp')
- wv: bfloat16 [2, 896, 896], P(None, 'dp')
- wo: bfloat16 [2, 896, 896], P(None, 'dp')
- w_gate: bfloat16 [2, 896, 3584], P(None, 'dp')
- w_up: bfloat16 [2, 896, 3584], P(None, 'dp')
- w_down: bfloat16 [2, 3584, 896], P(None, 'dp')
- m_wq: float32 [2, 896, 896], P(None, 'dp')
- m_wk: float32 [2, 896, 896], P(None, 'dp')
- m_wv: float32 [2, 896, 896], P(None, 'dp')
- m_wo: float32 [2, 896, 896], P(None, 'dp')
- m_w_gate: float32 [2, 896, 3584], P(None, 'dp')
- m_w_up: float32 [2, 896, 3584], P(None, 'dp')
- m_w_down: float32 [2, 3584, 896], P(None, 'dp')
- v_wq: float32 [2, 896, 896], P(None, 'dp')
- v_wk: float32 [2, 896, 896], P(None, 'dp')
- v_wv: float32 [2, 896, 896], P(None, 'dp')
- v_wo: float32 [2, 896, 896], P(None, 'dp')
- v_w_gate: float32 [2, 896, 3584], P(None, 'dp')
- v_w_up: float32 [2, 896, 3584], P(None, 'dp')
- v_w_down: float32 [2, 3584, 896], P(None, 'dp')
Outputs:
- output 1: bfloat16 [2, 896, 896], P('rep', 'dp')
- output 2: bfloat16 [2, 896, 896], P('rep', 'dp')
- output 3: bfloat16 [2, 896, 896], P('rep', 'dp')
- output 4: bfloat16 [2, 896, 896], P('rep', 'dp')
- output 5: bfloat16 [2, 896, 3584], P('rep', 'dp')
- output 6: bfloat16 [2, 896, 3584], P('rep', 'dp')
- output 7: bfloat16 [2, 3584, 896], P('rep', 'dp')
- output 8: float32 [2, 896, 896], P('rep', 'dp')
- output 9: float32 [2, 896, 896], P('rep', 'dp')
- output 10: float32 [2, 896, 896], P('rep', 'dp')
- output 11: float32 [2, 896, 896], P('rep', 'dp')
- output 12: float32 [2, 896, 3584], P('rep', 'dp')
- output 13: float32 [2, 896, 3584], P('rep', 'dp')
- output 14: float32 [2, 3584, 896], P('rep', 'dp')
- output 15: float32 [2, 896, 896], P('rep', 'dp')
- output 16: float32 [2, 896, 896], P('rep', 'dp')
- output 17: float32 [2, 896, 896], P('rep', 'dp')
- output 18: float32 [2, 896, 896], P('rep', 'dp')
- output 19: float32 [2, 896, 3584], P('rep', 'dp')
- output 20: float32 [2, 896, 3584], P('rep', 'dp')
- output 21: float32 [2, 3584, 896], P('rep', 'dp')
All inputs are finite; a program needn't handle non-finite values.
Results may differ from the reference program's by a relative error of at most 0.0269.
Values are sent between devices in bfloat16 or wider.
A program may use at most 768 MiB of HBM per device.

```python
import jax
import jax.numpy as jnp
from jax import lax

SEQUENCES = 32
TOKENS = 2048
D = 896
HEADS = 7
KV_HEADS = 7
HEAD = 128
FF = 3584
LAYERS = 2
THETA = 10000
NAMES = ("wq", "wk", "wv", "wo", "w_gate", "w_up", "w_down")
SHAPES = {
    "wq": (LAYERS, D, HEADS * HEAD),
    "wk": (LAYERS, D, KV_HEADS * HEAD),
    "wv": (LAYERS, D, KV_HEADS * HEAD),
    "wo": (LAYERS, HEADS * HEAD, D),
    "w_gate": (LAYERS, D, FF),
    "w_up": (LAYERS, D, FF),
    "w_down": (LAYERS, FF, D),
}


def bump(key, n, height):
    away = (jnp.arange(n, dtype=jnp.int32) - jax.random.randint(key, (), 0, n, jnp.int32)) % n
    return jnp.where(away < n // 8, height, 1.0)


def together(key, own, strength):
    shared = jax.random.normal(key, own.shape[1:], jnp.float32)
    return (own + strength * shared) * lax.rsqrt(1 + strength * strength)


def setup_inputs(seed: int = 0, part: int = 0) -> dict:
    kx, kdy, ka, kb, kz, kf, kh, kl, *keys = jax.random.split(jax.random.key(seed), 8 + 3 * len(NAMES))
    kx, kdy, ka, kb = (jax.random.fold_in(k, part) for k in (kx, kdy, ka, kb))
    kw, km, kv = (keys[i::3] for i in range(3))
    shape = (SEQUENCES, TOKENS, D)
    much_x, much_dy = jax.random.uniform(kz, (2,), jnp.float32, 0.0, 1.0)
    loud = 2.0 ** jax.random.uniform(jax.random.fold_in(kz, 1), (), jnp.float32, -1.0, 2.0)
    layers = 2.0 ** jax.random.uniform(kl, (LAYERS, 1, 1), jnp.float32, -1.0, 1.0)
    times = {"wq": 1.0, "wk": 1.0, "wv": 2.0, "wo": layers, "w_gate": 1.0, "w_up": bump(kh, FF, 4.0), "w_down": layers}
    x = together(ka, jax.random.normal(kx, shape, jnp.float32), much_x) * bump(kf, D, 4.0)
    dy = together(kb, jax.random.normal(kdy, shape, jnp.float32), much_dy)
    drawn = {"x": x.astype(jnp.bfloat16), "dy": (loud * dy * (SEQUENCES * TOKENS) ** -0.5).astype(jnp.bfloat16)}
    for key, name in zip(kw, NAMES, strict=True):
        drawn[name] = (jax.random.normal(key, SHAPES[name], jnp.float32) * SHAPES[name][1] ** -0.5 * times[name]).astype(jnp.bfloat16)
    for key, name in zip(km, NAMES, strict=True):
        drawn[f"m_{name}"] = 0.1 * jax.random.normal(key, SHAPES[name], jnp.float32)
    for key, name in zip(kv, NAMES, strict=True):
        drawn[f"v_{name}"] = jax.random.uniform(key, SHAPES[name], jnp.float32, 0.02, 0.06)
    return drawn


def matmul(a, w):
    return jnp.dot(a, w, preferred_element_type=jnp.float32).astype(jnp.bfloat16)


def normed(h):
    wide = h.astype(jnp.float32)
    scale = lax.rsqrt(jnp.mean(wide**2, -1, keepdims=True) + 1e-6)
    return (wide * scale).astype(jnp.bfloat16)


def turned(t, theta):
    half = t.shape[-1] // 2
    angle = jnp.arange(t.shape[0], dtype=jnp.float32)[:, None] * theta ** (-jnp.arange(half, dtype=jnp.float32) / half)
    cos, sin = jnp.cos(angle)[:, None], jnp.sin(angle)[:, None]
    a, b = t[..., :half].astype(jnp.float32), t[..., half:].astype(jnp.float32)
    return jnp.concatenate([a * cos - b * sin, b * cos + a * sin], -1).astype(jnp.bfloat16)


def seen_by(q, k, v):
    tokens, kv = q.shape[0], k.shape[1]
    q = q.reshape(tokens, kv, -1, q.shape[-1])
    scores = jnp.einsum("tgsd,ugd->gstu", q.astype(jnp.float32), k.astype(jnp.float32)) * q.shape[-1] ** -0.5
    place = jnp.arange(tokens)
    weights = jax.nn.softmax(jnp.where(place[:, None] >= place, scores, -jnp.inf), -1).astype(jnp.bfloat16)
    return jnp.einsum("gstu,ugd->tgsd", weights.astype(jnp.float32), v.astype(jnp.float32)).astype(jnp.bfloat16).reshape(tokens, -1)


def layer(h, w):
    a = normed(h)
    q, k = (turned(matmul(a, w[name]).reshape(h.shape[0], -1, HEAD), THETA) for name in ("wq", "wk"))
    h = h + matmul(seen_by(q, k, matmul(a, w["wv"]).reshape(h.shape[0], -1, HEAD)), w["wo"])
    b = normed(h)
    gate = jnp.dot(b, w["w_gate"], preferred_element_type=jnp.float32)
    up = jnp.dot(b, w["w_up"], preferred_element_type=jnp.float32)
    return h + matmul((jax.nn.silu(gate) * up).astype(jnp.bfloat16), w["w_down"])


def adamw(w, m, v, g):
    m = 0.9 * m + 0.1 * g
    v = 0.95 * v + 0.05 * g * g
    step = m * lax.rsqrt(v + 1e-8) + 0.1 * w
    return (w - 0.02 * step).astype(jnp.bfloat16), m, v


def clipped(gradients, sum_of_squares, count):
    factor = jnp.minimum(1.0, 0.5 * lax.rsqrt(sum_of_squares / count + 1e-30))
    return [g * factor for g in gradients]


def stack(weights, h):
    return lax.scan(lambda h, w: (layer(h, w), None), h, weights)[0]


def reference(x, dy, wq, wk, wv, wo, w_gate, w_up, w_down, m_wq, m_wk, m_wv, m_wo, m_w_gate, m_w_up, m_w_down, v_wq, v_wk, v_wv, v_wo, v_w_gate, v_w_up, v_w_down):
    weights = dict(zip(NAMES, (wq, wk, wv, wo, w_gate, w_up, w_down), strict=True))

    def take(so_far, sequence):
        h, by_y = sequence
        _, back = jax.vjp(stack, weights, h)
        by_weights, by_h = back(by_y)
        return jax.tree.map(lambda total, term: total + term.astype(jnp.float32), so_far, by_weights), by_h

    none_yet = {name: jnp.zeros(w.shape, jnp.float32) for name, w in weights.items()}
    by_weights, by_x = lax.scan(take, none_yet, (x, dy))
    gradients = [by_weights[name].astype(jnp.bfloat16).astype(jnp.float32) for name in NAMES]
    gradients = clipped(gradients, sum(jnp.sum(g * g) for g in gradients), sum(g.size for g in gradients))
    first = (m_wq, m_wk, m_wv, m_wo, m_w_gate, m_w_up, m_w_down)
    second = (v_wq, v_wk, v_wv, v_wo, v_w_gate, v_w_up, v_w_down)
    new = [adamw(weights[name].astype(jnp.float32), m, v, g) for name, m, v, g in zip(NAMES, first, second, gradients, strict=True)]
    return tuple(one[which] for which in range(3) for one in new)
```

```python
import functools
import math

import jax
import jax.numpy as jnp
import numpy as np
from jax import lax
from jax.experimental import pallas as pl
from jax.experimental.pallas import tpu as pltpu
from jax.sharding import PartitionSpec as P

ZERO, ONE, TWO = range(3)
HEAD = 128
LANES = 128
SUBLANES = 8
THETA = 10000
LOG2E = 1.4426950408889634
HIDDEN = -2e30
BLOCK = 512
PANEL = 1792
MIB = 2**20
F32, BF16 = jnp.float32, jnp.bfloat16
NN, NT, TN = ((1,), (0,)), ((1,), (1,)), ((0,), (0,))
IN_HBM = pl.BlockSpec(memory_space=pltpu.HBM)
IN_VMEM = pl.BlockSpec(memory_space=pltpu.VMEM)
MESH = pl.DeviceIdType.MESH


def mm(a, b, dims=NN):
    return lax.dot_general(a, b, (dims, ((), ())), preferred_element_type=F32)


def shape(dims, dtype=BF16):
    return jax.ShapeDtypeStruct(tuple(dims), dtype)


def params(vmem=60, **more):
    return pltpu.CompilerParams(vmem_limit_bytes=vmem * MIB, **more)


def cost(flops, *arrays):
    return pl.CostEstimate(flops=int(flops), transcendentals=0, bytes_accessed=sum(int(a.size) * a.dtype.itemsize for a in arrays))


def _seen():
    return lax.broadcasted_iota(jnp.int32, (BLOCK, BLOCK), 0) <= lax.broadcasted_iota(jnp.int32, (BLOCK, BLOCK), 1)


def _attend(q_ref, k_ref, v_ref, o_ref, lse_ref, values, *, scale):
    e = scale * LOG2E
    t, d = q_ref.shape[1:]
    values[:d, :] = v_ref[0].T
    values[d:, :] = jnp.ones((SUBLANES, t), BF16)
    seen = _seen()
    for a in range(0, t, BLOCK):
        n = a + BLOCK
        q = q_ref[0, a:n, :]
        spans = [(a, n, jnp.where(seen, mm(k_ref[0, a:n, :], q, NT), HIDDEN))]
        if a:
            spans.append((0, a, mm(k_ref[0, :a, :], q, NT)))
        top = functools.reduce(jnp.maximum, [s.max(0, keepdims=True) for _, _, s in spans])
        mix = sum(mm(values[:, x:y], jnp.exp2((s - top) * e).astype(BF16)) for x, y, s in spans)
        total = mix[d : d + 1]
        o_ref[0, a:n, :] = (mix[:d] * (1 / total)).T.astype(BF16)
        lse_ref[0, :, a:n] = top * scale + jnp.log(total)


def _attend_back(q_ref, k_ref, v_ref, do_ref, lse_ref, delta_ref, dq_ref, dk_ref, dv_ref, dq, *, scale):
    e = scale * LOG2E
    t = q_ref.shape[ONE]
    seen = _seen()
    lse, delta = lse_ref[ZERO] * LOG2E, delta_ref[ZERO]
    for a in range(ZERO, t, BLOCK):
        n = a + BLOCK
        k, v = k_ref[ZERO, a:n, :], v_ref[ZERO, a:n, :]
        turned = k.T
        dk = dv = 0.0
        for x, y in [(a, n)] + ([(n, t)] if n < t else []):
            s = mm(k, q_ref[ZERO, x:y, :], NT)
            dp = mm(v, do_ref[ZERO, x:y, :], NT)
            p = jnp.exp2(s * e - lse[:, x:y])
            if x == a:
                p = jnp.where(seen, p, 0.0)
            ds = (p * (dp - delta[:, x:y])).astype(BF16)
            dv += mm(p.astype(BF16), do_ref[ZERO, x:y, :])
            dk += mm(ds, q_ref[ZERO, x:y, :])
            part = mm(turned, ds)
            if a:
                dq[:, x:y] += part
            else:
                dq[:, x:y] = part
        dv_ref[ZERO, a:n, :] = dv.astype(BF16)
        dk_ref[ZERO, a:n, :] = (dk * scale).astype(BF16)
        dq_ref[ZERO, a:n, :] = (dq[:, a:n] * scale).T.astype(BF16)


def one_head(q, rows_of=None):
    dims = (1, *q.shape[1:]) if rows_of is None else (1, 1, q.shape[1])
    return pl.BlockSpec(dims, lambda i: (i, 0, 0))


def attend(q, k, v):
    n, t, d = q.shape
    spec, stat = one_head(q), one_head(q, True)
    return pl.pallas_call(
        functools.partial(_attend, scale=d**-0.5),
        grid=(n,),
        in_specs=[spec] * 3,
        out_specs=[spec, stat],
        out_shape=[shape(q.shape), shape((n, 1, t), F32)],
        scratch_shapes=[pltpu.VMEM((d + SUBLANES, t), BF16)],
        compiler_params=params(),
        cost_estimate=cost(4 * n * t * t * d, q, k, v, q),
        name="attend",
    )(q, k, v)


def attend_back(q, k, v, do, lse, delta):
    n, t, d = q.shape
    spec, stat = one_head(q), one_head(q, True)
    return pl.pallas_call(
        functools.partial(_attend_back, scale=d**-0.5),
        grid=(n,),
        in_specs=[spec] * 4 + [stat] * 2,
        out_specs=[spec] * 3,
        out_shape=[shape(q.shape)] * 3,
        scratch_shapes=[pltpu.VMEM((d, t), F32)],
        compiler_params=params(),
        cost_estimate=cost(10 * n * t * t * d, q, k, v, do, q, k, v),
        name="attend_back",
    )(q, k, v, do, lse, delta)


def flat(x):
    return x.reshape(-1, x.shape[-1])


def norm_parts(h):
    wide = h.astype(F32)
    return wide, lax.rsqrt(jnp.mean(wide * wide, -1, keepdims=True) + 1e-6)


def norm_back(by_a, wide, scale):
    by_a = by_a.astype(F32)
    dot = jnp.sum(by_a * wide, -1, keepdims=True)
    return by_a * scale - wide * (scale * scale * scale * (1 / wide.shape[-1]) * dot)


def joined(ref, a=0, n=None):
    n = ref.shape[1] if n is None else n
    return jnp.concatenate([ref[i, a : a + n] for i in range(ref.shape[0])], axis=1)


def rows(tile, width):
    return pl.BlockSpec((tile, width), lambda i: (i, 0))


def heads_of(n, tile):
    return pl.BlockSpec((n, tile, HEAD), lambda i: (0, i, 0))


def number(g, first, i):
    many, at = i
    return at // many * (g.shape[1] // 2) + first + at % many


def load(g, first, name, ref, n, sems):
    d, half = g.shape[3], n // TWO
    if name == "qkv":
        return [[pltpu.make_async_copy(g.at[:, number(g, first, (TWO, i))], ref.at[:, :, i * d : (i + ONE) * d], sems[ZERO]) for i in range(3)]]
    if name == "wo":
        return [[pltpu.make_async_copy(g.at[:, number(g, first, (TWO, 3))], ref, sems[ZERO])]]
    if name == "w_down":
        at = [(i, number(g, first + TWO * half, (half, i))) for i in (ZERO, half)]
        some = g.shape[ZERO] // TWO
        return [[pltpu.make_async_copy(g.at[pl.ds(c, some), pl.ds(b, half)], ref.at[pl.ds(c, some), pl.ds(i, half)], sem) for i, b in at]
                for c, sem in zip((ZERO, some), sems)]
    first += half if name == "w_up" else ZERO
    return [[pltpu.make_async_copy(g.at[:, number(g, first, (half, i))], ref.at[:, :, i * d : (i + ONE) * d], sem) for i in range(k, k + half)]
            for k, sem in zip((ZERO, half), sems)]


def at_first(groups):
    first = pl.program_id(0) == 0

    @pl.when(first)
    def _():
        for group in groups:
            for c in group:
                c.start()

    def ready(k):
        @pl.when(first)
        def _():
            for c in groups[k]:
                c.wait()

    return ready


def inner_weights(g_refs, firsts, refs, n, sem):
    wo, *inner = refs
    sems = sem.at[0], sem.at[1]
    halves = zip(*[load(g_refs[1], firsts[1], name, ref, n, sems) for name, ref in zip(("w_gate", "w_up", "w_down"), inner)])
    return at_first(load(g_refs[0], firsts[0], "wo", wo, n, [sem.at[2]]) + [sum(half, []) for half in halves])


def inner_scratch(g, n):
    chips, _, r, d = g.shape
    return [pltpu.VMEM((chips, r, d), BF16), pltpu.VMEM((chips, r, n * d), BF16), pltpu.VMEM((chips, r, n * d), BF16), pltpu.VMEM((chips, n, r, d), BF16),
            pltpu.SemaphoreType.DMA((3,))]


def _project(h_ref, cos_ref, sin_ref, g_ref, q_ref, k_ref, v_ref, w, sem, *, first):
    at_first(load(g_ref, first, "qkv", w, ZERO, [sem.at[ZERO]]))(ZERO)
    d = h_ref.shape[ONE]
    part = h_ref.shape[ZERO] // TWO
    for a in (ZERO, part):
        wide, scale = norm_parts(h_ref[a : a + part])
        t = mm((wide * scale).astype(BF16), flat(w[...])).astype(BF16)
        cos, sin = cos_ref[a : a + part], sin_ref[a : a + part]
        for n, ref in enumerate((q_ref, k_ref, v_ref)):
            for i in range(ref.shape[ZERO]):
                x = t[:, n * d + i * HEAD : n * d + (i + ONE) * HEAD]
                if n < TWO:
                    x = x.astype(F32)
                    x = (x * cos + pltpu.roll(x, HEAD // TWO, ONE) * sin).astype(BF16)
                ref[i, a : a + part] = x


def project(h, ga, tables, tile=512):
    g, first = ga
    tokens, d = h.shape
    chips, _, r, _ = g.shape
    n = d // HEAD
    out = shape((n, tokens, HEAD))
    return pl.pallas_call(
        functools.partial(_project, first=first),
        grid=(tokens // tile,),
        in_specs=[rows(tile, d), rows(tile, HEAD), rows(tile, HEAD), IN_HBM],
        out_specs=[heads_of(n, tile)] * 3,
        out_shape=[out] * 3,
        scratch_shapes=[pltpu.VMEM((chips, r, 3 * d), BF16), pltpu.SemaphoreType.DMA((1,))],
        compiler_params=params(),
        cost_estimate=cost(6 * tokens * d * d, h, out, out, out),
        name="project",
    )(h, *tables, g)


def _rest(h_ref, o_ref, ga_ref, gm_ref, h2_ref, b_ref, gate_ref, up_ref, act_ref, y_ref, wo, wg, wu, wd, sem, *, firsts):
    ready = inner_weights((ga_ref, gm_ref), firsts, (wo, wg, wu, wd), wd.shape[ONE], sem)
    ready(ZERO)
    h2 = h_ref[...] + mm(joined(o_ref), flat(wo[...])).astype(BF16)
    h2_ref[...] = h2
    wide, scale = norm_parts(h2)
    b = (wide * scale).astype(BF16)
    b_ref[...] = b
    total = 0.0
    w_down = lambda a: flat(wd[a // PANEL * (wd.shape[ZERO] // TWO) : (a // PANEL + ONE) * (wd.shape[ZERO] // TWO)])
    for a in range(ZERO, gate_ref.shape[ONE], PANEL):
        ready(ONE + a // PANEL)
        here = slice(a, a + PANEL)
        gate = mm(b, flat(wg[:, :, here]))
        up = mm(b, flat(wu[:, :, here]))
        gate_ref[:, here] = gate
        up_ref[:, here] = up
        act = (gate * jax.nn.sigmoid(gate) * up).astype(BF16)
        act_ref[:, here] = act
        total += mm(act, w_down(a))
    y_ref[...] = h2 + total.astype(BF16)


def rest(h, o, ga, gm, n, tile=256):
    tokens, d = h.shape
    f = n * d
    assert f == 2 * PANEL
    narrow = shape((tokens, d))
    return pl.pallas_call(
        functools.partial(_rest, firsts=(ga[1], gm[1])),
        grid=(tokens // tile,),
        in_specs=[rows(tile, d), heads_of(d // HEAD, tile), IN_HBM, IN_HBM],
        out_specs=[rows(tile, d)] * 2 + [rows(tile, f)] * 3 + [rows(tile, d)],
        out_shape=[narrow, narrow, shape((tokens, f), F32), shape((tokens, f), F32), shape((tokens, f)), narrow],
        scratch_shapes=inner_scratch(gm[0], n),
        compiler_params=params(),
        cost_estimate=cost(2 * tokens * d * (d + 3 * f), h, o, gm[0]),
        name="rest",
    )(h, o, ga[0], gm[0])


def _rest_back(*refs, last, firsts):
    if last:
        dy_ref, h_ref, o_ref, ga_ref, gm_ref, b_ref, act_ref, dgu_ref, dh_ref, do_ref, delta_ref, wo, wg, wu, wd, sem = refs
    else:
        dy_ref, h_ref, o_ref, gate_ref, up_ref, ga_ref, gm_ref, dgu_ref, dh_ref, do_ref, delta_ref, wo, wg, wu, wd, sem = refs
    ready = inner_weights((ga_ref, gm_ref), firsts, (wo, wg, wu, wd), wd.shape[ONE], sem)
    ready(ZERO)
    dy = dy_ref[...]
    h2 = h_ref[...]
    if last:
        h2 += mm(joined(o_ref), flat(wo[...])).astype(BF16)
    wide, scale = norm_parts(h2)
    if last:
        b = (wide * scale).astype(BF16)
        b_ref[...] = b
    f = dgu_ref.shape[ONE] // TWO
    total = 0.0
    for a in range(ZERO, f, PANEL):
        k = a // PANEL
        ready(ONE + k)
        here = slice(a, a + PANEL)
        w_gate, w_up = flat(wg[:, :, here]), flat(wu[:, :, here])
        some = wd.shape[ZERO] // TWO
        if last:
            gate, up = mm(b, w_gate), mm(b, w_up)
        else:
            gate, up = gate_ref[:, here], up_ref[:, here]
        d_act = mm(dy, flat(wd[k * some : (k + ONE) * some]), NT).astype(BF16).astype(F32)
        sig = jax.nn.sigmoid(gate)
        silu = gate * sig
        if last:
            act_ref[:, here] = (silu * up).astype(BF16)
        d_up = (d_act * silu).astype(BF16)
        d_gate = (d_act * up * (sig + silu * (ONE - sig))).astype(BF16)
        dgu_ref[:, here] = d_gate
        dgu_ref[:, f + a : f + a + PANEL] = d_up
        total += mm(d_gate, w_gate, NT) + mm(d_up, w_up, NT)
    dh = dy + norm_back(total.astype(BF16), wide, scale).astype(BF16)
    dh_ref[...] = dh
    do = mm(dh, flat(wo[...]), NT).astype(BF16)
    for i in range(do_ref.shape[ZERO]):
        part = do[:, i * HEAD : (i + ONE) * HEAD]
        do_ref[i] = part
        delta_ref[i] = jnp.sum((part.astype(F32) * o_ref[i].astype(F32)).T, axis=ZERO, keepdims=True)


def rest_back(dy, h, o, ga, gm, n, gate=None, up=None, tile=256):
    tokens, d = dy.shape
    f = n * d
    heads = d // HEAD
    last = gate is None
    narrow, wide = shape((tokens, d)), shape((tokens, f))
    given = [dy, h, o] + ([] if last else [gate, up]) + [ga[ZERO], gm[ZERO]]
    specs = [rows(tile, d), rows(tile, d), heads_of(heads, tile)] + ([] if last else [rows(tile, f)] * TWO) + [IN_HBM, IN_HBM]
    outs = [(rows(tile, d), narrow), (rows(tile, f), wide)] if last else []
    outs += [(rows(tile, TWO * f), shape((tokens, TWO * f))), (rows(tile, d), narrow), (heads_of(heads, tile), shape((heads, tokens, HEAD))),
             (pl.BlockSpec((heads, ONE, tile), lambda i: (ZERO, ZERO, i)), shape((heads, ONE, tokens), F32))]
    return pl.pallas_call(
        functools.partial(_rest_back, last=last, firsts=(ga[ONE], gm[ONE])),
        grid=(tokens // tile,),
        in_specs=specs,
        out_specs=[s for s, _ in outs],
        out_shape=[s for _, s in outs],
        scratch_shapes=inner_scratch(gm[ZERO], n),
        compiler_params=params(),
        cost_estimate=cost(TWO * tokens * d * ((TWO if last else ONE) * d + (5 if last else 3) * f), *given),
        name="rest_back_last" if last else "rest_back",
    )(*given)


def _weights_back(b_ref, dgu_ref, act_hbm, dy_hbm, o_hbm, dh_hbm, out_ref, out2_ref, bt, stage, act, dy, o, dh, sem, in_sem):
    s = pl.program_id(ZERO)
    chips, blocks, r, d = out_ref.shape
    n = blocks // 3
    half = n // TWO
    per = blocks // TWO
    early = 4
    late = [pltpu.make_async_copy(a, b, in_sem.at[i]) for i, (a, b) in enumerate(((dy_hbm, dy), (o_hbm, o), (dh_hbm, dh)))]
    acts = [pltpu.make_async_copy(act_hbm.at[:, pl.ds(k * d, d)], act.at[k % TWO], in_sem.at[3 + k % TWO]) for k in range(n)]

    def gate_up(k):
        which, core = divmod(k, TWO)
        return [pltpu.make_async_copy(stage.at[k % TWO, :, :, pl.ds(i * d, d)], out_ref.at[:, core * per + which * half + i], sem.at[k % TWO]) for i in range(half)]

    def down(k):
        some = chips // n
        src = stage.at[k % TWO, :, :, pl.ds(ZERO, d)]
        return [pltpu.make_async_copy(src.at[pl.ds(i * n + j, ONE)], out_ref.at[pl.ds(k * some + i, ONE), j // half * per + TWO * half + j % half], sem.at[k % TWO])
                for i in range(some) for j in range(n)]

    steps = [gate_up(k) for k in range(early)] + [down(k) for k in range(n)]
    steps.append([pltpu.make_async_copy(stage.at[ZERO, :, :, pl.ds(ZERO, d)], out2_ref.at[:, 3], sem.at[ZERO])])
    for k in range(len(steps)):
        @pl.when(s == k)
        def _(k=k):
            if k == ZERO:
                for c in late:
                    c.start()
            if k >= TWO:
                for c in steps[k - TWO]:
                    c.wait()
            if early - ONE <= k < early - ONE + n:
                acts[k - early + ONE].start()
            if k == early:
                late[ZERO].wait()
            if early <= k < early + n:
                acts[k - early].wait()
            if k == early + n:
                late[ONE].wait()
                late[TWO].wait()

    @pl.when(s == ZERO)
    def _():
        bt[...] = b_ref[...].T

    @pl.when(s < early)
    def _():
        stage[lax.rem(s, TWO)] = mm(bt[...], dgu_ref[...]).astype(BF16).reshape(chips, r, half * d)

    @pl.when((s >= early) & (s < early + n))
    def _():
        stage[lax.rem(s, TWO), :, :, :d] = mm(act[lax.rem(s, TWO)], dy[...], TN).astype(BF16).reshape(chips, r, d)

    @pl.when(s == early + n)
    def _():
        stage[ZERO, :, :, :d] = mm(joined(o), dh[...], TN).astype(BF16).reshape(chips, r, d)

    for k in range(len(steps)):
        @pl.when(s == k)
        def _(k=k):
            for c in steps[k]:
                c.start()
            if k == len(steps) - ONE:
                for c in steps[k - ONE] + steps[k]:
                    c.wait()


def weights_back(b, dgu, act, dy, o, dh, g, n):
    tokens, d = b.shape
    chips, _, r, _ = g.shape
    f = n * d
    panel = f // TWO
    return pl.pallas_call(
        _weights_back,
        grid=(4 + n + ONE,),
        in_specs=[pl.BlockSpec((tokens, d), lambda s: (ZERO, ZERO), pipeline_mode=pl.Buffered(ONE)), pl.BlockSpec((tokens, panel), lambda s: (ZERO, jnp.minimum(s, 3)))]
        + [IN_HBM] * 4,
        out_specs=[IN_HBM, IN_HBM],
        out_shape=[shape((chips, 3 * n, r, d)), shape((chips, 4, r, d))],
        scratch_shapes=[pltpu.VMEM((d, tokens), BF16), pltpu.VMEM((TWO, chips, r, panel), BF16), pltpu.VMEM((TWO, tokens, d), BF16), pltpu.VMEM((tokens, d), BF16),
                        pltpu.VMEM(o.shape, BF16), pltpu.VMEM((tokens, d), BF16), pltpu.SemaphoreType.DMA((TWO,)), pltpu.SemaphoreType.DMA((5,))],
        compiler_params=params(),
        cost_estimate=cost(TWO * tokens * d * (d + 3 * f), b, dgu, act, dy),
        name="weights_back",
    )(b, dgu, act, dy, o, dh)


def _project_back(*refs, last, first):
    if last:
        h_ref, dq_ref, dk_ref, dv_ref, cos_ref, sin_ref, _, out_ref, total, stage, sem = refs
    else:
        h_ref, dh_ref, dq_ref, dk_ref, dv_ref, cos_ref, sin_ref, g_ref, _, dx_ref, out_ref, total, stage, sem, w, wsem = refs
        at_first(load(g_ref, first, "qkv", w, ZERO, [wsem.at[ZERO]]))(ZERO)
    s = pl.program_id(ZERO)
    chips, _, r, d = out_ref.shape

    @pl.when(s == ZERO)
    def _():
        total[...] = jnp.zeros_like(total)

    wide, scale = norm_parts(h_ref[...])
    a = (wide * scale).astype(BF16)
    cos, sin = cos_ref[...], sin_ref[...]
    by_a = 0.0
    for n, ref in reversed(list(enumerate((dq_ref, dk_ref, dv_ref)))):
        parts = []
        for i in range(ref.shape[ZERO]):
            x = ref[i]
            if n < TWO:
                x = x.astype(F32)
                x = (x * cos - pltpu.roll(x, HEAD // TWO, ONE) * sin).astype(BF16)
            parts.append(x)
        t = jnp.concatenate(parts, axis=ONE)
        total[:, n * d : (n + ONE) * d] += mm(a, t, TN)
        if not last:
            by_a += mm(t, flat(w[:, :, n * d : (n + ONE) * d]), NT)
    if not last:
        dx_ref[...] = dh_ref[...] + norm_back(by_a.astype(BF16), wide, scale).astype(BF16)

    @pl.when(s == pl.num_programs(ZERO) - ONE)
    def _():
        done = [pltpu.make_async_copy(stage.at[:, :, pl.ds(i * d, d)], out_ref.at[:, i], sem.at[i]) for i in range(3)]
        for i in range(3):
            stage[:, :, i * d : (i + ONE) * d] = total[:, i * d : (i + ONE) * d].astype(BF16).reshape(chips, r, d)
            done[i].start()
        for c in done:
            c.wait()


def project_back(h, dh, dq, dk, dv, tables, ga, into, tile=512):
    tokens, d = h.shape
    n = d // HEAD
    last = dh is None
    chips, _, r, _ = into.shape
    given = [h] + ([] if last else [dh]) + [dq, dk, dv, *tables] + ([] if last else [ga[ZERO]]) + [into]
    specs = [rows(tile, d)] * (ONE if last else TWO) + [heads_of(n, tile)] * 3 + [rows(tile, HEAD)] * TWO + [IN_HBM] * (ONE if last else TWO)
    outs = ([] if last else [(rows(tile, d), shape((tokens, d)))]) + [(IN_HBM, shape(into.shape))]
    blocks = pltpu.VMEM((chips, r, 3 * d), BF16)
    scratch = [pltpu.VMEM((d, 3 * d), F32), blocks, pltpu.SemaphoreType.DMA((3,))] + ([] if last else [blocks, pltpu.SemaphoreType.DMA((ONE,))])
    return pl.pallas_call(
        functools.partial(_project_back, last=last, first=ga[ONE]),
        grid=(tokens // tile,),
        in_specs=specs,
        out_specs=[s for s, _ in outs],
        out_shape=[s for _, s in outs],
        scratch_shapes=scratch,
        input_output_aliases={len(given) - ONE: len(outs) - ONE},
        compiler_params=params(),
        cost_estimate=cost((ONE if last else TWO) * 6 * tokens * d * d, h, dq, dk, dv),
        name="project_back_last" if last else "project_back",
    )(*given)


class Place:
    def __init__(self, size):
        self.chips = size // 2
        self.side = math.isqrt(self.chips)
        me = lax.axis_index("dp")
        self.core = lax.rem(me, 2)
        chip = lax.div(me, 2)
        self.x, self.y = lax.div(chip, self.side), lax.rem(chip, self.side)
        self.other = dict(device_id={"dp": me + 1 - 2 * self.core}, device_id_type=MESH)

    def at(self, u, i, j):
        dx, dy = (j, i) if u else (i, j)
        wrap = lambda a: lax.rem(a + self.side, self.side)
        return wrap(self.x + dx) * self.side + wrap(self.y + dy)

    def to(self, u, i, j):
        return dict(device_id={"dp": self.at(u, i, j) * 2 + self.core}, device_id_type=MESH)

    def greet(self):
        barrier = pltpu.get_barrier_semaphore()
        peers = [self.other] + [self.to(0, i, j) for i, j in ((1, 0), (-1, 0), (0, 1), (0, -1))]
        for peer in peers:
            pl.semaphore_signal(barrier, inc=1, **peer)
        pl.semaphore_wait(barrier, len(peers))


CUT = 32


def _spread(own_ref, out_ref, out_sem, in_sem, over_out, over_in, own_sem, *, size):
    here = Place(size)
    far, back = here.side // TWO, here.side - ONE
    r = own_ref.shape[ONE]
    parts = (slice(ZERO, r), slice(ZERO, CUT), slice(CUT, r))
    keys = [(u, *k) for u in (ZERO, ONE) for k in
            [(ONE, ZERO, ZERO), (back, ZERO, ZERO), (far, ZERO, ONE), (far, ZERO, TWO)] + [(i, j, p) for i in range(here.side) for j, p in ((ONE, ZERO), (back, ZERO), (far, ONE), (far, TWO))]]

    def slot(u, i, j, p):
        return out_ref.at[here.at(u, -i, -j), here.core * TWO + u, parts[p]]

    started = []

    def send(u, i, j, p, step, key):
        k = keys.index((u, *key))
        src = own_ref.at[u] if (i, j) == (ZERO, ZERO) else slot(u, i, j, p)
        copy = pltpu.make_async_remote_copy(src, slot(u, i, j, p), out_sem.at[k], in_sem.at[k], **here.to(u, *step))
        copy.start()
        started.append(copy)

    def wait(u, *key):
        k = keys.index((u, *key))
        ref = slot(u, *key)
        pltpu.make_async_remote_copy(ref, ref, out_sem.at[k], in_sem.at[k], **here.to(u, ONE, ZERO)).wait_recv()

    def over(u, i, j):
        k = u * here.chips + i * here.side + j
        src = own_ref.at[u] if (i, j) == (ZERO, ZERO) else slot(u, i, j, ZERO)
        copy = pltpu.make_async_remote_copy(src, slot(u, i, j, ZERO), over_out.at[k], over_in.at[k], **here.other)
        copy.start()
        started.append(copy)

    def fan(u, i):
        send(u, i, ZERO, ZERO, (ZERO, ONE), (i, ONE, ZERO))
        send(u, i, ZERO, ZERO, (ZERO, -ONE), (i, back, ZERO))

    def second(u, i):
        wait(u, i, ONE, ZERO)
        send(u, i, ONE, ONE, (ZERO, ONE), (i, far, ONE))
        wait(u, i, back, ZERO)
        send(u, i, back, TWO, (ZERO, -ONE), (i, far, TWO))
        over(u, i, ONE)
        over(u, i, back)

    here.greet()
    for u in (ZERO, ONE):
        send(u, ZERO, ZERO, ZERO, (ONE, ZERO), (ONE, ZERO, ZERO))
        send(u, ZERO, ZERO, ZERO, (-ONE, ZERO), (back, ZERO, ZERO))
        fan(u, ZERO)
    mine = [pltpu.make_async_copy(own_ref.at[u], slot(u, ZERO, ZERO, ZERO), own_sem.at[u]) for u in (ZERO, ONE)]
    for u in (ZERO, ONE):
        over(u, ZERO, ZERO)
        mine[u].start()
    for u in (ZERO, ONE):
        wait(u, ONE, ZERO, ZERO)
        send(u, ONE, ZERO, ONE, (ONE, ZERO), (far, ZERO, ONE))
        fan(u, ONE)
        wait(u, back, ZERO, ZERO)
        send(u, back, ZERO, TWO, (-ONE, ZERO), (far, ZERO, TWO))
        fan(u, back)
    for u in (ZERO, ONE):
        over(u, ONE, ZERO)
        over(u, back, ZERO)
        second(u, ZERO)
    for u in (ZERO, ONE):
        wait(u, far, ZERO, ONE)
        wait(u, far, ZERO, TWO)
        fan(u, far)
        over(u, far, ZERO)
    for i in (ONE, back, far):
        for u in (ZERO, ONE):
            second(u, i)
    for i in (ZERO, ONE, back, far):
        for u in (ZERO, ONE):
            wait(u, i, far, ONE)
            wait(u, i, far, TWO)
            over(u, i, far)
    for c in mine:
        c.wait()
    for u in (ZERO, ONE):
        for k in range(here.chips):
            ref = out_ref.at[here.at(u, -(k // here.side), -(k % here.side)), (ONE - here.core) * TWO + u]
            pltpu.make_async_remote_copy(ref, ref, over_out.at[u * here.chips + k], over_in.at[u * here.chips + k], **here.other).wait_recv()
    for c in started:
        c.wait_send()


def spread(own, size):
    messages = 2 * (math.isqrt(size // 2) + 1) * 4
    dma = pltpu.SemaphoreType.DMA
    return pl.pallas_call(
        functools.partial(_spread, size=size),
        in_specs=[IN_HBM],
        out_specs=IN_HBM,
        out_shape=shape((size // 2, 4, *own.shape[1:])),
        scratch_shapes=[dma((messages,)), dma((messages,)), dma((size,)), dma((size,)), dma((2,))],
        compiler_params=params(16, collective_id=3, has_side_effects=True),
        cost_estimate=pl.CostEstimate(flops=10**10, transcendentals=0, bytes_accessed=10**7),
        name="spread",
    )(own)


def _collect(grads_ref, out_ref, own, sib, total, far_out, far_in, near_out, near_in, over_out, over_in, far_sem, near_sem, own_sem, *, size):
    here = Place(size)
    far, back = here.side // TWO, here.side - ONE
    r = grads_ref.shape[TWO]
    parts = ((slice(ZERO, CUT), (ZERO, ONE)), (slice(CUT, r), (ZERO, -ONE)))
    order = (far, ONE, back, ZERO)
    both = [(u, i) for i in order for u in (ZERO, ONE)]
    started, waiting = [], []

    def start(copies):
        flush()
        waiting.extend(copies)

    def flush():
        for c in waiting:
            c.start()
        started.extend(waiting)
        waiting.clear()

    mine = pltpu.make_async_copy(grads_ref.at[:, pl.ds(TWO * here.core, TWO)], own, own_sem)
    mine.start()
    here.greet()
    overs = {}
    for j in (far, ONE, back, ZERO):
        for u, i in both:
            k = u * here.chips + i * here.side + j
            overs[u, i, j] = pltpu.make_async_remote_copy(grads_ref.at[here.at(u, i, j), TWO * (ONE - here.core) + u], sib.at[k], over_out.at[k], over_in.at[k],
                                                          **here.other)
            overs[u, i, j].start()
    mine.wait()

    def ours(u, i, j):
        overs[u, i, j].wait_recv()
        return own[here.at(u, i, j), u].astype(F32) + sib[u * here.chips + i * here.side + j].astype(F32)

    def turn(u, i, step):
        return step if i < here.side else step[::-ONE]

    def first(u, i, block):
        far_out[u, i] = block.astype(BF16)
        start([pltpu.make_async_remote_copy(far_out.at[u, i, rows_], far_in.at[u, i, rows_], far_sem.at[ZERO, u, i, n], far_sem.at[ONE, u, i, n],
                                            **here.to(u, *turn(u, i, step))) for n, (rows_, step) in enumerate(parts)])

    def landed(sems, ref, u, i, n):
        pltpu.make_async_remote_copy(ref, ref, sems.at[ZERO, u, i, n], sems.at[ONE, u, i, n], **here.other).wait_recv()

    def second(u, i, block, n):
        rows_, step = parts[n]
        landed(far_sem, far_in.at[u, i, rows_], u, i, n)
        pieces = [block[:CUT], block[CUT:]]
        pieces[n] += far_in[u, i, rows_].astype(F32)
        near_out[u, i, n, :CUT] = pieces[ZERO].astype(BF16)
        near_out[u, i, n, CUT:] = pieces[ONE].astype(BF16)
        start([pltpu.make_async_remote_copy(near_out.at[u, i, n], near_in.at[u, i, n], near_sem.at[ZERO, u, i, n], near_sem.at[ONE, u, i, n],
                                            **here.to(u, *turn(u, i, step)))])

    def third(u, i, block):
        for n in (ZERO, ONE):
            landed(near_sem, near_in.at[u, i, n], u, i, n)
            block += near_in[u, i, n].astype(F32)
        return block

    for u, i in both:
        first(u, i, ours(u, i, far))
    for u, i in both:
        for n, j in enumerate((ONE, back)):
            second(u, i, ours(u, i, j), n)
    for u, i in both:
        block = third(u, i, ours(u, i, ZERO))
        if i == far:
            first(u, here.side, block)
        elif i:
            second(u, here.side, block, ZERO if i == ONE else ONE)
        else:
            total[u] = block
    flush()
    for u in (ZERO, ONE):
        out_ref[u] = third(u, here.side, total[u]).astype(BF16)
    for c in list(overs.values()) + started:
        c.wait_send()


def collect(grads, size):
    chips, _, r, d = grads.shape
    rings = math.isqrt(chips) + ONE
    dma, vmem = pltpu.SemaphoreType.DMA, pltpu.VMEM
    return pl.pallas_call(
        functools.partial(_collect, size=size),
        in_specs=[IN_HBM],
        out_specs=IN_VMEM,
        out_shape=shape((TWO, r, d)),
        scratch_shapes=[vmem((chips, TWO, r, d), BF16), vmem((size, r, d), BF16), vmem((TWO, r, d), F32), vmem((TWO, rings, r, d), BF16), vmem((TWO, rings, r, d), BF16),
                        vmem((TWO, rings, TWO, r, d), BF16), vmem((TWO, rings, TWO, r, d), BF16), dma((size,)), dma((size,)), dma((TWO, TWO, rings, TWO)),
                        dma((TWO, TWO, rings, TWO)), dma],
        compiler_params=params(32, collective_id=4, has_side_effects=True),
        cost_estimate=pl.CostEstimate(flops=10**10, transcendentals=ZERO, bytes_accessed=10**7),
        name="collect",
    )(grads)


def _pack(*refs, layers, n):
    weights, outs, (send, got, send_sem, got_sem) = refs[:7], refs[7 : 8 + layers], refs[8 + layers :]
    me = lax.axis_index("dp")
    core = lax.rem(me, TWO)
    other = dict(device_id={"dp": me + ONE - TWO * core}, device_id_type=MESH)
    half = n // TWO
    r, _, d = weights[ZERO].shape
    shared = TWO + TWO * half
    barrier = pltpu.get_barrier_semaphore()
    pl.semaphore_signal(barrier, inc=ONE, **other)

    def part(k, core, layer):
        if k < TWO:
            return weights[TWO * core + k][...].astype(F32)[:, layer].astype(BF16)
        which, i = divmod(k - TWO, half)
        i += core * half
        return weights[4 + which][:, :, i * d : (i + ONE) * d].astype(F32)[:, layer].astype(BF16)

    def into(k, layer):
        if k < TWO:
            return outs[layer], k if layer == ZERO else k + shared - TWO + half
        return outs[layer + ONE], k - TWO

    def each(do):
        for layer in range(layers):
            for k in range(shared):
                do(k, layer)

    def fill(core):
        def give(k, layer):
            send[layer, k] = part(k, ONE - core, layer)

        def keep(k, layer):
            out, at = into(k, layer)
            out[at, core * r : (core + ONE) * r] = part(k, core, layer)

        each(give)
        each(keep)

    def fill_rest(core):
        def take(k, layer):
            out, at = into(k, layer)
            out[at, (ONE - core) * r : (TWO - core) * r] = got[layer, k]

        each(take)

    for c in (ZERO, ONE):
        pl.when(core == c)(functools.partial(fill, c))
    pl.semaphore_wait(barrier, ONE)
    copy = pltpu.make_async_remote_copy(send, got, send_sem, got_sem, **other)
    copy.start()
    for layer in range(layers):
        for i in range(half):
            outs[layer + ONE][TWO * half + i] = weights[6][layer, i * TWO * r : (i + ONE) * TWO * r]
    copy.wait()
    for c in (ZERO, ONE):
        pl.when(core == c)(functools.partial(fill_rest, c))


def pack(weights, n):
    r, layers, d = weights[ZERO].shape
    half = n // TWO
    blocks = [TWO] + [3 * half + TWO] * (layers - ONE) + [3 * half]
    return pl.pallas_call(
        functools.partial(_pack, layers=layers, n=n),
        in_specs=[IN_VMEM] * 7,
        out_specs=[IN_VMEM] * len(blocks),
        out_shape=[shape((k, TWO * r, d)) for k in blocks],
        scratch_shapes=[pltpu.VMEM((layers, TWO + TWO * half, r, d), BF16)] * TWO + [pltpu.SemaphoreType.DMA] * TWO,
        compiler_params=params(32, collective_id=TWO, has_side_effects=True),
        cost_estimate=pl.CostEstimate(flops=10**8, transcendentals=ZERO, bytes_accessed=10**6),
        name="pack",
    )(*weights)


def _meet(*refs, size):
    n = (len(refs) - 7) // TWO
    grads, (total_ref, *got), (part, parts, out_sem, in_sem, swap_out, swap_in) = refs[:n], refs[n : TWO * n + ONE], refs[TWO * n + ONE :]
    me = lax.axis_index("dp")
    other = dict(device_id={"dp": me + ONE - TWO * lax.rem(me, TWO)}, device_id_type=MESH)
    peer = lambda i: dict(device_id={"dp": lax.rem(me + i, size)}, device_id_type=MESH)
    barrier = pltpu.get_barrier_semaphore()
    for i in range(ONE, size):
        pl.semaphore_signal(barrier, inc=ONE, **peer(i))
    total = jnp.zeros((SUBLANES, LANES), F32)
    for ref in grads:
        x = ref[...].astype(F32)
        x = jnp.sum(x * x, axis=ZERO)
        x = sum(x[i : i + SUBLANES] for i in range(ZERO, x.shape[ZERO], SUBLANES))
        total += sum(x[:, i : i + LANES] for i in range(ZERO, x.shape[ONE], LANES))
    part[...] = total
    pl.semaphore_wait(barrier, size - ONE)
    swaps = [pltpu.make_async_remote_copy(ref.at[pl.ds(ZERO, to.shape[ZERO])], to, swap_out.at[i], swap_in.at[i], **other)
             for i, (ref, to) in enumerate(zip(grads, got))]
    for c in swaps:
        c.start()
    sends = [pltpu.make_async_remote_copy(part, parts.at[i], out_sem.at[i], in_sem.at[i], **peer(i)) for i in range(ONE, size)]
    for c in sends:
        c.start()
    parts[ZERO] = part[...]
    for c in sends:
        c.wait()
    total_ref[...] = lax.fori_loop(ZERO, size, lambda j, t: t + parts[lax.rem(me - j + size, size)], jnp.zeros_like(total))
    for c in swaps:
        c.wait()


def meet(grads, shared, size):
    n = len(grads)
    dma = pltpu.SemaphoreType.DMA
    return pl.pallas_call(
        functools.partial(_meet, size=size),
        in_specs=[IN_VMEM] * n,
        out_specs=[IN_VMEM] * (1 + n),
        out_shape=[shape((SUBLANES, LANES), F32)] + [shape((k, *x.shape[1:])) for k, x in zip(shared, grads)],
        scratch_shapes=[pltpu.VMEM((SUBLANES, LANES), F32), pltpu.VMEM((size, SUBLANES, LANES), F32), dma((size,)), dma((size,)), dma((n,)), dma((n,))],
        compiler_params=params(32, collective_id=1, has_side_effects=True),
        cost_estimate=pl.CostEstimate(flops=10**9, transcendentals=0, bytes_accessed=10**6),
        name="meet",
    )(*grads)


def _finish(total_ref, *refs, layers, count):
    grads = [refs[i * layers : (i + ONE) * layers] for i in range(4)]
    refs = refs[4 * layers :]
    weights, ms, vs, new_w, new_m, new_v, (narrow, wide) = (refs[i : i + 7] for i in range(ZERO, 43, 7))
    factor = jnp.minimum(1.0, 0.5 * lax.rsqrt(jnp.full((ONE, ONE), jnp.sum(total_ref[...])) / count + 1e-30))
    r, _, d = weights[ZERO].shape
    half = grads[ONE][ZERO].shape[ZERO] - grads[3][ZERO].shape[ZERO]
    core = lax.rem(lax.axis_index("dp"), TWO)

    def update(j, here, g):
        g = g * factor
        m = 0.9 * ms[j][here] + 0.1 * g
        v = 0.95 * vs[j][here] + 0.05 * g * g
        w = weights[j][here].astype(F32)
        new_m[j][here] = m
        new_v[j][here] = v
        new_w[j][here] = (w - 0.02 * (m * lax.rsqrt(v + 1e-8) + 0.1 * w)).astype(BF16)

    def lay(first):
        low, high = ((ZERO, ONE), (TWO, 3))[:: ONE if first else -ONE]
        at = slice(ZERO, r) if first else slice(r, TWO * r)
        for n in range(layers):
            for k in range(TWO):
                narrow[k, :, n, :] = grads[low[ZERO]][n][k, at].astype(F32)
                narrow[TWO + k, :, n, :] = grads[high[ZERO]][n][k, at].astype(F32)
                for i in range(half):
                    wide[k, :, n, i * d : (i + ONE) * d] = grads[low[ONE]][n][k * half + i, at].astype(F32)
                    wide[k, :, n, (half + i) * d : (half + i + ONE) * d] = grads[high[ONE]][n][k * half + i, at].astype(F32)

    for c in (ZERO, ONE):
        pl.when(core == c)(functools.partial(lay, c == ZERO))
    for j in range(4):
        update(j, ..., narrow[j])
    for j in range(TWO):
        for i in range(TWO * half):
            here = (slice(None), slice(None), slice(i * d, (i + ONE) * d))
            update(4 + j, here, wide[(j, *here)])
    for n in range(layers):
        for i in range(half):
            update(6, (n, slice(i * TWO * r, (i + ONE) * TWO * r)), grads[ONE][n][TWO * half + i].astype(F32))


def finish(total, grads, arrays, count):
    layers = len(grads[0])
    given = [total] + [x for some in grads for x in some] + list(arrays)
    outs = [shape(a.shape, a.dtype) for a in arrays]
    r, _, d = arrays[0].shape
    f = arrays[4].shape[2]
    return pl.pallas_call(
        functools.partial(_finish, layers=layers, count=count),
        in_specs=[IN_VMEM] * len(given),
        out_specs=[IN_VMEM] * len(outs),
        out_shape=outs,
        scratch_shapes=[pltpu.VMEM((4, r, layers, d), F32), pltpu.VMEM((2, r, layers, f), F32)],
        compiler_params=params(),
        cost_estimate=cost(10**7, *given, *outs),
        name="finish",
    )(*given)


def rotary(tokens):
    half = HEAD // 2
    angle = np.arange(tokens, dtype=np.float32)[:, None] * np.float32(THETA) ** (-np.arange(half, dtype=np.float32) / np.float32(half))
    cos, sin = np.cos(angle), np.sin(angle)
    return np.concatenate([cos, cos], 1), np.concatenate([-sin, sin], 1)


def solution(mesh):
    size = mesh.shape["dp"]
    chips = size // TWO

    def gathered(blocks):
        k, r, d = blocks.shape
        return lax.all_gather(blocks.reshape(k * r, d), "dp", axis=ZERO, tiled=True).reshape(chips, TWO * k, r, d)

    def scattered(blocks):
        _, k, r, d = blocks.shape
        return lax.psum_scatter(blocks.reshape(-ONE, d), "dp", scatter_dimension=ZERO, tiled=True).reshape(k // TWO, r, d)

    def turn(some):
        return [w.transpose(ONE, ZERO, TWO) for w in some[:6]] + [some[6]]

    def step(x, dy, *arrays):
        weights, m, v = (arrays[i : i + 7] for i in (ZERO, 7, 14))
        layers = weights[ZERO].shape[ZERO]
        h, dy = x[ZERO], dy[ZERO]
        tokens, d = h.shape
        n = weights[4].shape[TWO] // d
        per = 3 * (n // TWO)
        tables = rotary(tokens)

        own, *others = pack(turn(weights), n)
        later = [gathered(t) for t in others]
        ga = [(spread(own, size), ZERO)] + [(g, per) for g in later[:-ONE]]
        gm = [(g, ZERO) for g in later]
        kept = []
        for i in range(layers):
            q, k, v_ = project(h, ga[i], tables)
            o, lse = attend(q, k, v_)
            kept.append((h, q, k, v_, o, lse))
            if i < layers - ONE:
                h2, b, gate, up, act, h = rest(h, o, ga[i], gm[i], n)
                kept[i] += (h2, b, gate, up, act)
        pairs, inners = [None] * layers, [None] * layers
        for i in reversed(range(layers)):
            h, q, k, v_, o, lse, *more = kept[i]
            if i == layers - ONE:
                b, act, dgu, dh, do, delta = rest_back(dy, h, o, ga[i], gm[i], n)
            else:
                h2, b, gate, up, act = more
                dgu, dh, do, delta = rest_back(dy, h2, o, ga[i], gm[i], n, gate, up)
                dgu, inners[i + ONE] = lax.optimization_barrier((dgu, inners[i + ONE]))
            inner, into = weights_back(b, dgu, act, dy, o, dh, gm[i][ZERO], n)
            do, inner = lax.optimization_barrier((do, inner))
            inners[i] = scattered(inner)
            if i < layers - ONE:
                do, pairs[i + ONE] = lax.optimization_barrier((do, pairs[i + ONE]))
            dq, dk, dv = attend_back(q, k, v_, do, lse, delta)
            if i:
                dy, into = project_back(h, dh, dq, dk, dv, tables, ga[i], into)
                pairs[i] = scattered(into)
            else:
                (into,) = project_back(h, None, dq, dk, dv, tables, ga[i], into)
                pairs[i] = collect(into, size)
        grads = pairs + inners
        total, *got = meet(grads, [t.shape[ZERO] for t in pairs] + [t.shape[ZERO] - n // TWO for t in inners], size)
        done = finish(total, [pairs, inners, got[:layers], got[layers:]], turn(weights) + turn(m) + turn(v), size * sum(w.size for w in weights))
        return tuple(t for i in (ZERO, 7, 14) for t in turn(done[i : i + 7]))

    states, cut = P(("rep", "dp"), None, None), P(None, "dp", None)
    return jax.shard_map(
        step,
        mesh=mesh,
        in_specs=(states, states) + (cut,) * 21,
        out_specs=(P("rep", "dp", None),) * 21,
        check_vma=False,
    )
```

```python
import functools
import math

import jax
import jax.numpy as jnp
import numpy as np
from jax import lax
from jax.experimental import pallas as pl
from jax.experimental.pallas import tpu as pltpu
from jax.sharding import PartitionSpec as P

ZERO, ONE, TWO = range(3)
HEAD = 128
LANES = 128
SUBLANES = 8
THETA = 10000
LOG2E = 1.4426950408889634
HIDDEN = -2e30
BLOCK = 512
PANEL = 1792
MIB = 2**20
F32, BF16 = jnp.float32, jnp.bfloat16
NN, NT, TN = ((1,), (0,)), ((1,), (1,)), ((0,), (0,))
IN_HBM = pl.BlockSpec(memory_space=pltpu.HBM)
IN_VMEM = pl.BlockSpec(memory_space=pltpu.VMEM)
MESH = pl.DeviceIdType.MESH


def mm(a, b, dims=NN):
    return lax.dot_general(a, b, (dims, ((), ())), preferred_element_type=F32)


def shape(dims, dtype=BF16):
    return jax.ShapeDtypeStruct(tuple(dims), dtype)


def params(vmem=60, **more):
    return pltpu.CompilerParams(vmem_limit_bytes=vmem * MIB, **more)


def cost(flops, *arrays):
    return pl.CostEstimate(flops=int(flops), transcendentals=0, bytes_accessed=sum(int(a.size) * a.dtype.itemsize for a in arrays))


def _seen():
    return lax.broadcasted_iota(jnp.int32, (BLOCK, BLOCK), 0) <= lax.broadcasted_iota(jnp.int32, (BLOCK, BLOCK), 1)


def _attend(q_ref, k_ref, v_ref, o_ref, lse_ref, values, *, scale):
    e = scale * LOG2E
    t, d = q_ref.shape[1:]
    values[:d, :] = v_ref[0].T
    values[d:, :] = jnp.ones((SUBLANES, t), BF16)
    seen = _seen()
    for a in range(0, t, BLOCK):
        n = a + BLOCK
        q = q_ref[0, a:n, :]
        s = mm(k_ref[0, :n, :], q, NT)
        parts = ([s[:a]] if a else []) + [jnp.where(seen, s[a:], HIDDEN)]
        top = functools.reduce(jnp.maximum, [s.max(0, keepdims=True) for s in parts])
        mix = mm(values[:, :n], jnp.concatenate([jnp.exp2((s - top) * e).astype(BF16) for s in parts], axis=0))
        total = mix[d : d + 1]
        o_ref[0, a:n, :] = (mix[:d] * (1 / total)).T.astype(BF16)
        lse_ref[0, :, a:n] = top * scale + jnp.log(total)


def _attend_back(q_ref, k_ref, v_ref, do_ref, lse_ref, delta_ref, dq_ref, dk_ref, dv_ref, dq, *, scale):
    e = scale * LOG2E
    t = q_ref.shape[ONE]
    seen = _seen()
    lse, delta = lse_ref[ZERO] * LOG2E, delta_ref[ZERO]
    for a in range(ZERO, t, BLOCK):
        n = a + BLOCK
        k, v = k_ref[ZERO, a:n, :], v_ref[ZERO, a:n, :]
        turned = k.T
        s = mm(k, q_ref[ZERO, a:, :], NT)
        dp = mm(v, do_ref[ZERO, a:, :], NT)
        p = jnp.exp2(s * e - lse[:, a:])
        masked = jnp.where(seen, p[:, :BLOCK], 0.0)
        p = jnp.concatenate([masked, p[:, BLOCK:]], axis=ONE) if n < t else masked
        ds = (p * (dp - delta[:, a:])).astype(BF16)
        dv = mm(p.astype(BF16), do_ref[ZERO, a:, :])
        dk = mm(ds, q_ref[ZERO, a:, :])
        part = mm(turned, ds)
        if a:
            dq[:, a:] += part
        else:
            dq[...] = part
        dv_ref[ZERO, a:n, :] = dv.astype(BF16)
        dk_ref[ZERO, a:n, :] = (dk * scale).astype(BF16)
        dq_ref[ZERO, a:n, :] = (dq[:, a:n] * scale).T.astype(BF16)


def one_head(q, rows_of=None):
    dims = (1, *q.shape[1:]) if rows_of is None else (1, 1, q.shape[1])
    return pl.BlockSpec(dims, lambda i: (i, 0, 0))


def attend(q, k, v):
    n, t, d = q.shape
    spec, stat = one_head(q), one_head(q, True)
    return pl.pallas_call(
        functools.partial(_attend, scale=d**-0.5),
        grid=(n,),
        in_specs=[spec] * 3,
        out_specs=[spec, stat],
        out_shape=[shape(q.shape), shape((n, 1, t), F32)],
        scratch_shapes=[pltpu.VMEM((d + SUBLANES, t), BF16)],
        compiler_params=params(),
        cost_estimate=cost(4 * n * t * t * d, q, k, v, q),
        name="attend",
    )(q, k, v)


def attend_back(q, k, v, do, lse, delta):
    n, t, d = q.shape
    spec, stat = one_head(q), one_head(q, True)
    return pl.pallas_call(
        functools.partial(_attend_back, scale=d**-0.5),
        grid=(n,),
        in_specs=[spec] * 4 + [stat] * 2,
        out_specs=[spec] * 3,
        out_shape=[shape(q.shape)] * 3,
        scratch_shapes=[pltpu.VMEM((d, t), F32)],
        compiler_params=params(),
        cost_estimate=cost(10 * n * t * t * d, q, k, v, do, q, k, v),
        name="attend_back",
    )(q, k, v, do, lse, delta)


def flat(x):
    return x.reshape(-1, x.shape[-1])


def norm_parts(h):
    wide = h.astype(F32)
    return wide, lax.rsqrt(jnp.mean(wide * wide, -1, keepdims=True) + 1e-6)


def norm_back(by_a, wide, scale):
    by_a = by_a.astype(F32)
    dot = jnp.sum(by_a * wide, -1, keepdims=True)
    return by_a * scale - wide * (scale * scale * scale * (1 / wide.shape[-1]) * dot)


def joined(ref):
    return jnp.concatenate([ref[i] for i in range(ref.shape[0])], axis=1)


def rows(tile, width):
    return pl.BlockSpec((tile, width), lambda i: (i, 0))


def heads_of(n, tile):
    return pl.BlockSpec((n, tile, HEAD), lambda i: (0, i, 0))


def number(g, first, i):
    many, at = i
    return at // many * (g.shape[1] // 2) + first + at % many


def load(g, first, name, ref, n, sems):
    d, half = g.shape[3], n // TWO
    if name == "qkv":
        return [[pltpu.make_async_copy(g.at[:, number(g, first, (TWO, i))], ref.at[:, :, i * d : (i + ONE) * d], sems[ZERO]) for i in range(3)]]
    if name == "wo":
        return [[pltpu.make_async_copy(g.at[:, number(g, first, (TWO, 3))], ref, sems[ZERO])]]
    if name == "w_down":
        at = [(i, number(g, first + TWO * half, (half, i))) for i in (ZERO, half)]
        some = g.shape[ZERO] // TWO
        return [[pltpu.make_async_copy(g.at[pl.ds(c, some), pl.ds(b, half)], ref.at[pl.ds(c, some), pl.ds(i, half)], sem) for i, b in at]
                for c, sem in zip((ZERO, some), sems)]
    first += half if name == "w_up" else ZERO
    return [[pltpu.make_async_copy(g.at[:, number(g, first, (half, i))], ref.at[:, :, i * d : (i + ONE) * d], sem) for i in range(k, k + half)]
            for k, sem in zip((ZERO, half), sems)]


def at_first(groups):
    first = pl.program_id(0) == 0

    @pl.when(first)
    def _():
        for group in groups:
            for c in group:
                c.start()

    def ready(k):
        @pl.when(first)
        def _():
            for c in groups[k]:
                c.wait()

    return ready


def inner_weights(g_refs, firsts, refs, n, sem):
    wo, *inner = refs
    sems = sem.at[0], sem.at[1]
    halves = zip(*[load(g_refs[1], firsts[1], name, ref, n, sems) for name, ref in zip(("w_gate", "w_up", "w_down"), inner)])
    return at_first(load(g_refs[0], firsts[0], "wo", wo, n, [sem.at[2]]) + [sum(half, []) for half in halves])


def inner_scratch(g, n):
    chips, _, r, d = g.shape
    return [pltpu.VMEM((chips, r, d), BF16), pltpu.VMEM((chips, r, n * d), BF16), pltpu.VMEM((chips, r, n * d), BF16), pltpu.VMEM((chips, n, r, d), BF16),
            pltpu.SemaphoreType.DMA((3,))]


def _project(h_ref, cos_ref, sin_ref, g_ref, q_ref, k_ref, v_ref, w, sem, *, first):
    at_first(load(g_ref, first, "qkv", w, ZERO, [sem.at[ZERO]]))(ZERO)
    d = h_ref.shape[ONE]
    wide, scale = norm_parts(h_ref[...])
    t = mm((wide * scale).astype(BF16), flat(w[...])).astype(BF16)
    cos, sin = cos_ref[...], sin_ref[...]
    for n, ref in enumerate((q_ref, k_ref, v_ref)):
        for i in range(ref.shape[ZERO]):
            x = t[:, n * d + i * HEAD : n * d + (i + ONE) * HEAD]
            if n < TWO:
                x = x.astype(F32)
                x = (x * cos + pltpu.roll(x, HEAD // TWO, ONE) * sin).astype(BF16)
            ref[i] = x


def project(h, ga, tables, tile=512):
    g, first = ga
    tokens, d = h.shape
    chips, _, r, _ = g.shape
    n = d // HEAD
    out = shape((n, tokens, HEAD))
    return pl.pallas_call(
        functools.partial(_project, first=first),
        grid=(tokens // tile,),
        in_specs=[rows(tile, d), rows(tile, HEAD), rows(tile, HEAD), IN_HBM],
        out_specs=[heads_of(n, tile)] * 3,
        out_shape=[out] * 3,
        scratch_shapes=[pltpu.VMEM((chips, r, 3 * d), BF16), pltpu.SemaphoreType.DMA((1,))],
        compiler_params=params(),
        cost_estimate=cost(6 * tokens * d * d, h, out, out, out),
        name="project",
    )(h, *tables, g)


def _rest(h_ref, o_ref, ga_ref, gm_ref, h2_ref, b_ref, gate_ref, up_ref, act_ref, y_ref, wo, wg, wu, wd, sem, *, firsts):
    ready = inner_weights((ga_ref, gm_ref), firsts, (wo, wg, wu, wd), wd.shape[ONE], sem)
    ready(ZERO)
    h2 = h_ref[...] + mm(joined(o_ref), flat(wo[...])).astype(BF16)
    h2_ref[...] = h2
    wide, scale = norm_parts(h2)
    b = (wide * scale).astype(BF16)
    b_ref[...] = b
    total = 0.0
    w_down = lambda a: flat(wd[a // PANEL * (wd.shape[ZERO] // TWO) : (a // PANEL + ONE) * (wd.shape[ZERO] // TWO)])
    for a in range(ZERO, gate_ref.shape[ONE], PANEL):
        ready(ONE + a // PANEL)
        here = slice(a, a + PANEL)
        gate = mm(b, flat(wg[:, :, here]))
        up = mm(b, flat(wu[:, :, here]))
        gate_ref[:, here] = gate
        up_ref[:, here] = up
        act = (gate * jax.nn.sigmoid(gate) * up).astype(BF16)
        act_ref[:, here] = act
        total += mm(act, w_down(a))
    y_ref[...] = h2 + total.astype(BF16)


def rest(h, o, ga, gm, n, tile=256):
    tokens, d = h.shape
    f = n * d
    assert f == 2 * PANEL
    narrow = shape((tokens, d))
    return pl.pallas_call(
        functools.partial(_rest, firsts=(ga[1], gm[1])),
        grid=(tokens // tile,),
        in_specs=[rows(tile, d), heads_of(d // HEAD, tile), IN_HBM, IN_HBM],
        out_specs=[rows(tile, d)] * 2 + [rows(tile, f)] * 3 + [rows(tile, d)],
        out_shape=[narrow, narrow, shape((tokens, f), F32), shape((tokens, f), F32), shape((tokens, f)), narrow],
        scratch_shapes=inner_scratch(gm[0], n),
        compiler_params=params(),
        cost_estimate=cost(2 * tokens * d * (d + 3 * f), h, o, gm[0]),
        name="rest",
    )(h, o, ga[0], gm[0])


def _rest_back(*refs, last, firsts):
    if last:
        dy_ref, h_ref, o_ref, ga_ref, gm_ref, b_ref, act_ref, dgu_ref, dh_ref, do_ref, delta_ref, wo, wg, wu, wd, sem = refs
    else:
        dy_ref, h_ref, o_ref, gate_ref, up_ref, ga_ref, gm_ref, dgu_ref, dh_ref, do_ref, delta_ref, wo, wg, wu, wd, sem = refs
    ready = inner_weights((ga_ref, gm_ref), firsts, (wo, wg, wu, wd), wd.shape[ONE], sem)
    ready(ZERO)
    dy = dy_ref[...]
    h2 = h_ref[...]
    if last:
        h2 += mm(joined(o_ref), flat(wo[...])).astype(BF16)
    wide, scale = norm_parts(h2)
    if last:
        b = (wide * scale).astype(BF16)
        b_ref[...] = b
    f = dgu_ref.shape[ONE] // TWO
    total = 0.0
    for a in range(ZERO, f, PANEL):
        k = a // PANEL
        ready(ONE + k)
        here = slice(a, a + PANEL)
        w_gate, w_up = flat(wg[:, :, here]), flat(wu[:, :, here])
        some = wd.shape[ZERO] // TWO
        if last:
            gate, up = mm(b, w_gate), mm(b, w_up)
        else:
            gate, up = gate_ref[:, here], up_ref[:, here]
        d_act = mm(dy, flat(wd[k * some : (k + ONE) * some]), NT).astype(BF16).astype(F32)
        sig = jax.nn.sigmoid(gate)
        silu = gate * sig
        if last:
            act_ref[:, here] = (silu * up).astype(BF16)
        d_up = (d_act * silu).astype(BF16)
        d_gate = (d_act * up * (sig + silu * (ONE - sig))).astype(BF16)
        dgu_ref[:, here] = d_gate
        dgu_ref[:, f + a : f + a + PANEL] = d_up
        total += mm(d_gate, w_gate, NT) + mm(d_up, w_up, NT)
    dh = dy + norm_back(total.astype(BF16), wide, scale).astype(BF16)
    dh_ref[...] = dh
    do = mm(dh, flat(wo[...]), NT).astype(BF16)
    for i in range(do_ref.shape[ZERO]):
        part = do[:, i * HEAD : (i + ONE) * HEAD]
        do_ref[i] = part
        delta_ref[i] = jnp.sum((part.astype(F32) * o_ref[i].astype(F32)).T, axis=ZERO, keepdims=True)


def rest_back(dy, h, o, ga, gm, n, gate=None, up=None, tile=256):
    tokens, d = dy.shape
    f = n * d
    heads = d // HEAD
    last = gate is None
    narrow, wide = shape((tokens, d)), shape((tokens, f))
    given = [dy, h, o] + ([] if last else [gate, up]) + [ga[ZERO], gm[ZERO]]
    specs = [rows(tile, d), rows(tile, d), heads_of(heads, tile)] + ([] if last else [rows(tile, f)] * TWO) + [IN_HBM, IN_HBM]
    outs = [(rows(tile, d), narrow), (rows(tile, f), wide)] if last else []
    outs += [(rows(tile, TWO * f), shape((tokens, TWO * f))), (rows(tile, d), narrow), (heads_of(heads, tile), shape((heads, tokens, HEAD))),
             (pl.BlockSpec((heads, ONE, tile), lambda i: (ZERO, ZERO, i)), shape((heads, ONE, tokens), F32))]
    return pl.pallas_call(
        functools.partial(_rest_back, last=last, firsts=(ga[ONE], gm[ONE])),
        grid=(tokens // tile,),
        in_specs=specs,
        out_specs=[s for s, _ in outs],
        out_shape=[s for _, s in outs],
        scratch_shapes=inner_scratch(gm[ZERO], n),
        compiler_params=params(),
        cost_estimate=cost(TWO * tokens * d * ((TWO if last else ONE) * d + (5 if last else 3) * f), *given),
        name="rest_back_last" if last else "rest_back",
    )(*given)


def _weights_back(b_ref, dgu_ref, act_hbm, dy_hbm, o_hbm, dh_hbm, out_ref, out2_ref, bt, stage, act, dy, o, dh, sem, in_sem, *, panels):
    s = pl.program_id(ZERO)
    chips, blocks, r, d = out_ref.shape
    n = panels
    half = n // TWO
    per = blocks // TWO
    downs = n if per > TWO * half else ZERO
    early = 4
    late = [pltpu.make_async_copy(a, b, in_sem.at[i]) for i, (a, b) in enumerate(((o_hbm, o), (dh_hbm, dh)) + (((dy_hbm, dy),) if downs else ()))]
    acts = [pltpu.make_async_copy(act_hbm.at[:, pl.ds(k * d, d)], act.at[k % TWO], in_sem.at[3 + k % TWO]) for k in range(downs)]

    def gate_up(k):
        which, core = divmod(k, TWO)
        return [pltpu.make_async_copy(stage.at[k % TWO, :, :, pl.ds(i * d, d)], out_ref.at[:, core * per + which * half + i], sem.at[k % TWO]) for i in range(half)]

    def down(k):
        some = chips // n
        src = stage.at[k % TWO, :, :, pl.ds(ZERO, d)]
        return [pltpu.make_async_copy(src.at[pl.ds(i * n + j, ONE)], out_ref.at[pl.ds(k * some + i, ONE), j // half * per + TWO * half + j % half], sem.at[k % TWO])
                for i in range(some) for j in range(n)]

    steps = [gate_up(k) for k in range(early)] + [down(k) for k in range(downs)]
    last = early + downs
    steps.append([pltpu.make_async_copy(stage.at[ZERO, :, :, pl.ds(ZERO, d)], out2_ref.at[:, out2_ref.shape[ONE] // TWO + ONE], sem.at[ZERO])])
    for k in range(len(steps)):
        @pl.when(s == k)
        def _(k=k):
            if k == ZERO:
                for c in late:
                    c.start()
            if k >= TWO:
                for c in steps[k - TWO]:
                    c.wait()
            if early - ONE <= k < last - ONE:
                acts[k - early + ONE].start()
            if k == early and downs:
                late[TWO].wait()
            if early <= k < last:
                acts[k - early].wait()
            if k == last:
                late[ZERO].wait()
                late[ONE].wait()

    @pl.when(s == ZERO)
    def _():
        bt[...] = b_ref[...].T

    @pl.when(s < early)
    def _():
        stage[lax.rem(s, TWO)] = mm(bt[...], dgu_ref[...]).astype(BF16).reshape(chips, r, half * d)

    if downs:
        @pl.when((s >= early) & (s < last))
        def _():
            stage[lax.rem(s, TWO), :, :, :d] = mm(act[lax.rem(s, TWO)], dy[...], TN).astype(BF16).reshape(chips, r, d)

    @pl.when(s == last)
    def _():
        stage[ZERO, :, :, :d] = mm(joined(o), dh[...], TN).astype(BF16).reshape(chips, r, d)

    for k in range(len(steps)):
        @pl.when(s == k)
        def _(k=k):
            for c in steps[k]:
                c.start()
            if k == len(steps) - ONE:
                for c in steps[k - ONE] + steps[k]:
                    c.wait()


def weights_back(b, dgu, act, dy, o, dh, g, n, down, others):
    tokens, d = b.shape
    chips, _, r, _ = g.shape
    f = n * d
    panel = f // TWO
    return pl.pallas_call(
        functools.partial(_weights_back, panels=n),
        grid=(4 + (n if down else ZERO) + ONE,),
        in_specs=[pl.BlockSpec((tokens, d), lambda s: (ZERO, ZERO), pipeline_mode=pl.Buffered(ONE)), pl.BlockSpec((tokens, panel), lambda s: (ZERO, jnp.minimum(s, 3)))]
        + [IN_HBM] * 4,
        out_specs=[IN_HBM, IN_HBM],
        out_shape=[shape((chips, (3 if down else TWO) * n, r, d)), shape((chips, others, r, d))],
        scratch_shapes=[pltpu.VMEM((d, tokens), BF16), pltpu.VMEM((TWO, chips, r, panel), BF16), pltpu.VMEM((TWO, tokens, d), BF16), pltpu.VMEM((tokens, d), BF16),
                        pltpu.VMEM(o.shape, BF16), pltpu.VMEM((tokens, d), BF16), pltpu.SemaphoreType.DMA((TWO,)), pltpu.SemaphoreType.DMA((5,))],
        compiler_params=params(),
        cost_estimate=cost(TWO * tokens * d * (d + (3 if down else TWO) * f), b, dgu, act, dy),
        name="weights_back" if down else "weights_back_some",
    )(b, dgu, act, dy, o, dh)


def _down_back(act_ref, dy_ref, _, out_ref, stage, sem, *, panels):
    k = pl.program_id(0)
    chips, blocks, r, d = out_ref.shape
    some, half = chips // panels, panels // 2

    def copies(k):
        return [pltpu.make_async_copy(stage.at[k % 2, pl.ds(i * panels + j, 1)], out_ref.at[pl.ds(k * some + i, 1), j // half * (blocks // 2) + 2 + j % half], sem.at[k % 2])
                for i in range(some) for j in range(panels)]

    for a in range(2, panels):
        @pl.when(k == a)
        def _(a=a):
            for c in copies(a - 2):
                c.wait()

    stage[lax.rem(k, 2)] = mm(act_ref[...], dy_ref[...], TN).astype(BF16).reshape(chips, r, d)
    for a in range(panels):
        @pl.when(k == a)
        def _(a=a):
            for c in copies(a):
                c.start()
            if a == panels - 1:
                for c in copies(a - 1) + copies(a):
                    c.wait()


def down_back(act, dy, into, n):
    tokens, d = dy.shape
    chips, _, r, _ = into.shape
    return pl.pallas_call(
        functools.partial(_down_back, panels=n),
        grid=(n,),
        in_specs=[pl.BlockSpec((tokens, d), lambda s: (0, s)), pl.BlockSpec((tokens, d), lambda s: (0, 0), pipeline_mode=pl.Buffered(1)), IN_HBM],
        out_specs=IN_HBM,
        out_shape=shape(into.shape),
        scratch_shapes=[pltpu.VMEM((2, chips, r, d), BF16), pltpu.SemaphoreType.DMA((2,))],
        input_output_aliases={2: 0},
        compiler_params=params(),
        cost_estimate=cost(2 * tokens * d * n * d, act, dy),
        name="down_back",
    )(act, dy, into)


def _project_back(*refs, last, first):
    if last:
        h_ref, dq_ref, dk_ref, dv_ref, cos_ref, sin_ref, _, out_ref, total, stage, sem = refs
    else:
        h_ref, dh_ref, dq_ref, dk_ref, dv_ref, cos_ref, sin_ref, g_ref, _, dx_ref, out_ref, total, stage, sem, w, wsem = refs
        at_first(load(g_ref, first, "qkv", w, ZERO, [wsem.at[ZERO]]))(ZERO)
    s = pl.program_id(ZERO)
    chips, blocks, r, d = out_ref.shape

    @pl.when(s == ZERO)
    def _():
        total[...] = jnp.zeros_like(total)

    wide, scale = norm_parts(h_ref[...])
    a = (wide * scale).astype(BF16)
    cos, sin = cos_ref[...], sin_ref[...]
    def back(ref):
        x = ref.astype(F32)
        return (x * cos - pltpu.roll(x, HEAD // TWO, ONE) * sin).astype(BF16)

    parts = [[dv_ref[i] for i in range(dv_ref.shape[ZERO])]] + [[back(ref[i]) for i in range(ref.shape[ZERO])] for ref in (dq_ref, dk_ref)]
    parts = [jnp.concatenate(p, axis=ONE) for p in parts[ONE:] + parts[:ONE]]
    if last:
        for i in (TWO, ZERO, ONE):
            total[:, i * d : (i + ONE) * d] += mm(a, parts[i], TN)
    else:
        t = jnp.concatenate(parts, axis=ONE)
        total[...] += mm(a, t, TN)
        by_a = mm(t, flat(w[...]), NT)
        dx_ref[...] = dh_ref[...] + norm_back(by_a.astype(BF16), wide, scale).astype(BF16)

    @pl.when(s == pl.num_programs(ZERO) - ONE)
    def _():
        done = [pltpu.make_async_copy(stage.at[:, :, pl.ds(i * d, d)], out_ref.at[:, i // TWO * (blocks // TWO) + i % TWO], sem.at[i]) for i in range(3)]
        for i in range(3):
            stage[:, :, i * d : (i + ONE) * d] = total[:, i * d : (i + ONE) * d].astype(BF16).reshape(chips, r, d)
            done[i].start()
        for c in done:
            c.wait()


def project_back(h, dh, dq, dk, dv, tables, ga, into, tile=512):
    tokens, d = h.shape
    n = d // HEAD
    last = dh is None
    chips, _, r, _ = into.shape
    given = [h] + ([] if last else [dh]) + [dq, dk, dv, *tables] + ([] if last else [ga[ZERO]]) + [into]
    specs = [rows(tile, d)] * (ONE if last else TWO) + [heads_of(n, tile)] * 3 + [rows(tile, HEAD)] * TWO + [IN_HBM] * (ONE if last else TWO)
    outs = ([] if last else [(rows(tile, d), shape((tokens, d)))]) + [(IN_HBM, shape(into.shape))]
    blocks = pltpu.VMEM((chips, r, 3 * d), BF16)
    scratch = [pltpu.VMEM((d, 3 * d), F32), blocks, pltpu.SemaphoreType.DMA((3,))] + ([] if last else [blocks, pltpu.SemaphoreType.DMA((ONE,))])
    return pl.pallas_call(
        functools.partial(_project_back, last=last, first=ga[ONE]),
        grid=(tokens // tile,),
        in_specs=specs,
        out_specs=[s for s, _ in outs],
        out_shape=[s for _, s in outs],
        scratch_shapes=scratch,
        input_output_aliases={len(given) - ONE: len(outs) - ONE},
        compiler_params=params(),
        cost_estimate=cost((ONE if last else TWO) * 6 * tokens * d * d, h, dq, dk, dv),
        name="project_back_last" if last else "project_back",
    )(*given)


class Place:
    def __init__(self, size):
        self.chips = size // 2
        self.side = math.isqrt(self.chips)
        me = lax.axis_index("dp")
        self.core = lax.rem(me, 2)
        chip = lax.div(me, 2)
        self.x, self.y = lax.div(chip, self.side), lax.rem(chip, self.side)
        self.other = dict(device_id={"dp": me + 1 - 2 * self.core}, device_id_type=MESH)

    def at(self, u, i, j):
        dx, dy = (j, i) if u else (i, j)
        wrap = lambda a: lax.rem(a + self.side, self.side)
        return wrap(self.x + dx) * self.side + wrap(self.y + dy)

    def to(self, u, i, j):
        return dict(device_id={"dp": self.at(u, i, j) * 2 + self.core}, device_id_type=MESH)

    def greet(self):
        barrier = pltpu.get_barrier_semaphore()
        peers = [self.other] + [self.to(0, i, j) for i, j in ((1, 0), (-1, 0), (0, 1), (0, -1))]
        for peer in peers:
            pl.semaphore_signal(barrier, inc=1, **peer)
        pl.semaphore_wait(barrier, len(peers))


CUT = 32


def _spread(own_ref, out_ref, out_sem, in_sem, over_out, over_in, own_sem, *, size):
    here = Place(size)
    far, back = here.side // TWO, here.side - ONE
    r = own_ref.shape[ONE]
    parts = (slice(ZERO, r), slice(ZERO, CUT), slice(CUT, r))
    keys = [(u, *k) for u in (ZERO, ONE) for k in
            [(ONE, ZERO, ZERO), (back, ZERO, ZERO), (far, ZERO, ONE), (far, ZERO, TWO)] + [(i, j, p) for i in range(here.side) for j, p in ((ONE, ZERO), (back, ZERO), (far, ONE), (far, TWO))]]

    def slot(u, i, j, p):
        return out_ref.at[here.at(u, -i, -j), here.core * TWO + u, parts[p]]

    started = []

    def send(u, i, j, p, step, key):
        k = keys.index((u, *key))
        src = own_ref.at[u] if (i, j) == (ZERO, ZERO) else slot(u, i, j, p)
        copy = pltpu.make_async_remote_copy(src, slot(u, i, j, p), out_sem.at[k], in_sem.at[k], **here.to(u, *step))
        copy.start()
        started.append(copy)

    def wait(u, *key):
        k = keys.index((u, *key))
        ref = slot(u, *key)
        pltpu.make_async_remote_copy(ref, ref, out_sem.at[k], in_sem.at[k], **here.to(u, ONE, ZERO)).wait_recv()

    def over(u, i, j):
        k = u * here.chips + i * here.side + j
        src = own_ref.at[u] if (i, j) == (ZERO, ZERO) else slot(u, i, j, ZERO)
        copy = pltpu.make_async_remote_copy(src, slot(u, i, j, ZERO), over_out.at[k], over_in.at[k], **here.other)
        copy.start()
        started.append(copy)

    def fan(u, i):
        send(u, i, ZERO, ZERO, (ZERO, ONE), (i, ONE, ZERO))
        send(u, i, ZERO, ZERO, (ZERO, -ONE), (i, back, ZERO))

    def second(u, i):
        wait(u, i, ONE, ZERO)
        send(u, i, ONE, ONE, (ZERO, ONE), (i, far, ONE))
        wait(u, i, back, ZERO)
        send(u, i, back, TWO, (ZERO, -ONE), (i, far, TWO))
        over(u, i, ONE)
        over(u, i, back)

    here.greet()
    for u in (ZERO, ONE):
        send(u, ZERO, ZERO, ZERO, (ONE, ZERO), (ONE, ZERO, ZERO))
        send(u, ZERO, ZERO, ZERO, (-ONE, ZERO), (back, ZERO, ZERO))
        fan(u, ZERO)
    mine = [pltpu.make_async_copy(own_ref.at[u], slot(u, ZERO, ZERO, ZERO), own_sem.at[u]) for u in (ZERO, ONE)]
    for u in (ZERO, ONE):
        over(u, ZERO, ZERO)
        mine[u].start()
    for u in (ZERO, ONE):
        wait(u, ONE, ZERO, ZERO)
        send(u, ONE, ZERO, ONE, (ONE, ZERO), (far, ZERO, ONE))
        fan(u, ONE)
        wait(u, back, ZERO, ZERO)
        send(u, back, ZERO, TWO, (-ONE, ZERO), (far, ZERO, TWO))
        fan(u, back)
    for u in (ZERO, ONE):
        over(u, ONE, ZERO)
        over(u, back, ZERO)
        second(u, ZERO)
    for u in (ZERO, ONE):
        wait(u, far, ZERO, ONE)
        wait(u, far, ZERO, TWO)
        fan(u, far)
        over(u, far, ZERO)
    for i in (ONE, back, far):
        for u in (ZERO, ONE):
            second(u, i)
    for i in (ZERO, ONE, back, far):
        for u in (ZERO, ONE):
            wait(u, i, far, ONE)
            wait(u, i, far, TWO)
            over(u, i, far)
    for c in mine:
        c.wait()
    for u in (ZERO, ONE):
        for k in range(here.chips):
            ref = out_ref.at[here.at(u, -(k // here.side), -(k % here.side)), (ONE - here.core) * TWO + u]
            pltpu.make_async_remote_copy(ref, ref, over_out.at[u * here.chips + k], over_in.at[u * here.chips + k], **here.other).wait_recv()
    for c in started:
        c.wait_send()


def spread(own, size):
    messages = 2 * (math.isqrt(size // 2) + 1) * 4
    dma = pltpu.SemaphoreType.DMA
    return pl.pallas_call(
        functools.partial(_spread, size=size),
        in_specs=[IN_HBM],
        out_specs=IN_HBM,
        out_shape=shape((size // 2, 4, *own.shape[1:])),
        scratch_shapes=[dma((messages,)), dma((messages,)), dma((size,)), dma((size,)), dma((2,))],
        compiler_params=params(60, collective_id=3, has_side_effects=True),
        cost_estimate=pl.CostEstimate(flops=10**10, transcendentals=0, bytes_accessed=10**7),
        name="spread",
    )(own)


def _collect(grads_ref, out_ref, own, sib, total, far_out, far_in, near_out, near_in, over_out, over_in, far_sem, near_sem, own_sem, *, size):
    here = Place(size)
    far, back = here.side // TWO, here.side - ONE
    r = grads_ref.shape[TWO]
    parts = ((slice(ZERO, CUT), (ZERO, ONE)), (slice(CUT, r), (ZERO, -ONE)))
    order = (far, ONE, back, ZERO)
    both = [(u, i) for i in order for u in (ZERO, ONE)]
    started, waiting = [], []

    def start(copies):
        flush()
        waiting.extend(copies)

    def flush():
        for c in waiting:
            c.start()
        started.extend(waiting)
        waiting.clear()

    mine = pltpu.make_async_copy(grads_ref.at[:, pl.ds(TWO * here.core, TWO)], own, own_sem)
    mine.start()
    here.greet()
    overs = {}
    for j in (far, ONE, back, ZERO):
        for u, i in both:
            k = u * here.chips + i * here.side + j
            overs[u, i, j] = pltpu.make_async_remote_copy(grads_ref.at[here.at(u, i, j), TWO * (ONE - here.core) + u], sib.at[k], over_out.at[k], over_in.at[k],
                                                          **here.other)
            overs[u, i, j].start()
    mine.wait()

    def ours(u, i, j):
        overs[u, i, j].wait_recv()
        return own[here.at(u, i, j), u].astype(F32) + sib[u * here.chips + i * here.side + j].astype(F32)

    def turn(u, i, step):
        return step if i < here.side else step[::-ONE]

    def first(u, i, block):
        far_out[u, i] = block.astype(BF16)
        start([pltpu.make_async_remote_copy(far_out.at[u, i, rows_], far_in.at[u, i, rows_], far_sem.at[ZERO, u, i, n], far_sem.at[ONE, u, i, n],
                                            **here.to(u, *turn(u, i, step))) for n, (rows_, step) in enumerate(parts)])

    def landed(sems, ref, u, i, n):
        pltpu.make_async_remote_copy(ref, ref, sems.at[ZERO, u, i, n], sems.at[ONE, u, i, n], **here.other).wait_recv()

    def second(u, i, block, n):
        rows_, step = parts[n]
        landed(far_sem, far_in.at[u, i, rows_], u, i, n)
        pieces = [block[:CUT], block[CUT:]]
        pieces[n] += far_in[u, i, rows_].astype(F32)
        near_out[u, i, n, :CUT] = pieces[ZERO].astype(BF16)
        near_out[u, i, n, CUT:] = pieces[ONE].astype(BF16)
        start([pltpu.make_async_remote_copy(near_out.at[u, i, n], near_in.at[u, i, n], near_sem.at[ZERO, u, i, n], near_sem.at[ONE, u, i, n],
                                            **here.to(u, *turn(u, i, step)))])

    def third(u, i, block):
        for n in (ZERO, ONE):
            landed(near_sem, near_in.at[u, i, n], u, i, n)
            block += near_in[u, i, n].astype(F32)
        return block

    for u, i in both:
        first(u, i, ours(u, i, far))
    for u, i in both:
        for n, j in enumerate((ONE, back)):
            second(u, i, ours(u, i, j), n)
    for u, i in both:
        block = third(u, i, ours(u, i, ZERO))
        if i == far:
            first(u, here.side, block)
        elif i:
            second(u, here.side, block, ZERO if i == ONE else ONE)
        else:
            total[u] = block
    flush()
    for u in (ZERO, ONE):
        out_ref[u] = third(u, here.side, total[u]).astype(BF16)
    for c in list(overs.values()) + started:
        c.wait_send()


def collect(grads, size):
    chips, _, r, d = grads.shape
    rings = math.isqrt(chips) + ONE
    dma, vmem = pltpu.SemaphoreType.DMA, pltpu.VMEM
    return pl.pallas_call(
        functools.partial(_collect, size=size),
        in_specs=[IN_HBM],
        out_specs=IN_VMEM,
        out_shape=shape((TWO, r, d)),
        scratch_shapes=[vmem((chips, TWO, r, d), BF16), vmem((size, r, d), BF16), vmem((TWO, r, d), F32), vmem((TWO, rings, r, d), BF16), vmem((TWO, rings, r, d), BF16),
                        vmem((TWO, rings, TWO, r, d), BF16), vmem((TWO, rings, TWO, r, d), BF16), dma((size,)), dma((size,)), dma((TWO, TWO, rings, TWO)),
                        dma((TWO, TWO, rings, TWO)), dma],
        compiler_params=params(60, collective_id=4, has_side_effects=True),
        cost_estimate=pl.CostEstimate(flops=10**10, transcendentals=ZERO, bytes_accessed=10**7),
        name="collect",
    )(grads)


def _pack(*refs, layers, n):
    given, outs, weights, (send, got, send_sem, got_sem, sem) = refs[:7], refs[7 : 8 + layers], refs[8 + layers : 15 + layers], refs[15 + layers :]
    loads = [pltpu.make_async_copy(a, b, sem.at[i]) for i, (a, b) in enumerate(zip(given, weights))]
    for c in loads:
        c.start()
    me = lax.axis_index("dp")
    core = lax.rem(me, TWO)
    other = dict(device_id={"dp": me + ONE - TWO * core}, device_id_type=MESH)
    half = n // TWO
    r, _, d = weights[ZERO].shape
    shared = TWO + TWO * half
    barrier = pltpu.get_barrier_semaphore()
    pl.semaphore_signal(barrier, inc=ONE, **other)

    def part(k, core, layer):
        if k < TWO:
            return weights[TWO * core + k][...].astype(F32)[:, layer].astype(BF16)
        which, i = divmod(k - TWO, half)
        i += core * half
        return weights[4 + which][:, :, i * d : (i + ONE) * d].astype(F32)[:, layer].astype(BF16)

    def into(k, layer):
        if k < TWO:
            return outs[layer], k if layer == ZERO else k + shared - TWO + half
        return outs[layer + ONE], k - TWO

    def each(do):
        for layer in range(layers):
            for k in range(shared):
                do(k, layer)

    def fill(core):
        def give(k, layer):
            send[layer, k] = part(k, ONE - core, layer)

        def keep(k, layer):
            out, at = into(k, layer)
            out[at, core * r : (core + ONE) * r] = part(k, core, layer)

        each(give)
        each(keep)

    def fill_rest(core):
        def take(k, layer):
            out, at = into(k, layer)
            out[at, (ONE - core) * r : (TWO - core) * r] = got[layer, k]

        each(take)

    for c in loads:
        c.wait()
    for c in (ZERO, ONE):
        pl.when(core == c)(functools.partial(fill, c))
    pl.semaphore_wait(barrier, ONE)
    copy = pltpu.make_async_remote_copy(send, got, send_sem, got_sem, **other)
    copy.start()
    for layer in range(layers):
        for i in range(half):
            outs[layer + ONE][TWO * half + i] = weights[6][layer, i * TWO * r : (i + ONE) * TWO * r]
    copy.wait()
    for c in (ZERO, ONE):
        pl.when(core == c)(functools.partial(fill_rest, c))


def pack(weights, n):
    r, layers, d = weights[ZERO].shape
    half = n // TWO
    blocks = [TWO] + [3 * half + TWO] * (layers - ONE) + [3 * half]
    return pl.pallas_call(
        functools.partial(_pack, layers=layers, n=n),
        in_specs=[IN_HBM] * 7,
        out_specs=[IN_VMEM] * len(blocks),
        out_shape=[shape((k, TWO * r, d)) for k in blocks],
        scratch_shapes=[pltpu.VMEM(w.shape, BF16) for w in weights] + [pltpu.VMEM((layers, TWO + TWO * half, r, d), BF16)] * TWO
        + [pltpu.SemaphoreType.DMA] * TWO + [pltpu.SemaphoreType.DMA((7,))],
        compiler_params=params(60, collective_id=TWO, has_side_effects=True),
        cost_estimate=pl.CostEstimate(flops=10**8, transcendentals=ZERO, bytes_accessed=10**6),
        name="pack",
    )(*weights)


def _meet(*refs, size, n, shared):
    grads, (total_ref, *got), (part, parts, out_sem, in_sem, swap_out, swap_in) = refs[:n], refs[n : n + shared + ONE], refs[n + shared + ONE :]
    me = lax.axis_index("dp")
    other = dict(device_id={"dp": me + ONE - TWO * lax.rem(me, TWO)}, device_id_type=MESH)
    peer = lambda i: dict(device_id={"dp": lax.rem(me + i, size)}, device_id_type=MESH)
    barrier = pltpu.get_barrier_semaphore()
    for i in range(ONE, size):
        pl.semaphore_signal(barrier, inc=ONE, **peer(i))
    total = jnp.zeros((SUBLANES, LANES), F32)
    for ref in grads:
        x = ref[...].astype(F32)
        x = jnp.sum(x * x, axis=ZERO)
        x = sum(x[i : i + SUBLANES] for i in range(ZERO, x.shape[ZERO], SUBLANES))
        total += sum(x[:, i : i + LANES] for i in range(ZERO, x.shape[ONE], LANES))
    part[...] = total
    pl.semaphore_wait(barrier, size - ONE)
    swaps = [pltpu.make_async_remote_copy(ref, to, swap_out.at[i], swap_in.at[i], **other)
             for i, (ref, to) in enumerate(zip(grads, got))]
    for c in swaps:
        c.start()
    sends = [pltpu.make_async_remote_copy(part, parts.at[i], out_sem.at[i], in_sem.at[i], **peer(i)) for i in range(ONE, size)]
    for c in sends:
        c.start()
    parts[ZERO] = part[...]
    for c in sends:
        c.wait()
    total_ref[...] = lax.fori_loop(ZERO, size, lambda j, t: t + parts[lax.rem(me - j + size, size)], jnp.zeros_like(total))
    for c in swaps:
        c.wait()


def meet(grads, shared, size):
    n = len(grads)
    dma = pltpu.SemaphoreType.DMA
    return pl.pallas_call(
        functools.partial(_meet, size=size, n=n, shared=shared),
        in_specs=[IN_VMEM] * n,
        out_specs=[IN_VMEM] * (1 + shared),
        out_shape=[shape((SUBLANES, LANES), F32)] + [shape(x.shape) for x in grads[:shared]],
        scratch_shapes=[pltpu.VMEM((SUBLANES, LANES), F32), pltpu.VMEM((size, SUBLANES, LANES), F32), dma((size,)), dma((size,)), dma((shared,)), dma((shared,))],
        compiler_params=params(60, collective_id=1, has_side_effects=True),
        cost_estimate=pl.CostEstimate(flops=10**9, transcendentals=0, bytes_accessed=10**6),
        name="meet",
    )(*grads)


def _finish(total_ref, *refs, layers, count):
    grads = [refs[i * layers : (i + ONE) * layers] for i in range(5)]
    refs = refs[5 * layers :]
    weights, ms, vs, new_w, new_m, new_v, (narrow, wide) = (refs[i : i + 7] for i in range(ZERO, 43, 7))
    factor = jnp.minimum(1.0, 0.5 * lax.rsqrt(jnp.full((ONE, ONE), jnp.sum(total_ref[...])) / count + 1e-30))
    r, _, d = weights[ZERO].shape
    half = grads[4][ZERO].shape[ZERO]
    core = lax.rem(lax.axis_index("dp"), TWO)

    def update(j, here, g):
        g = g * factor
        m = 0.9 * ms[j][here] + 0.1 * g
        v = 0.95 * vs[j][here] + 0.05 * g * g
        w = weights[j][here].astype(F32)
        new_m[j][here] = m
        new_v[j][here] = v
        new_w[j][here] = (w - 0.02 * (m * lax.rsqrt(v + 1e-8) + 0.1 * w)).astype(BF16)

    def lay(first):
        low, high = ((ZERO, ONE), (TWO, 3))[:: ONE if first else -ONE]
        at = slice(ZERO, r) if first else slice(r, TWO * r)
        for n in range(layers):
            for k in range(TWO):
                narrow[k, :, n, :] = grads[low[ZERO]][n][k, at].astype(F32)
                narrow[TWO + k, :, n, :] = grads[high[ZERO]][n][k, at].astype(F32)
                for i in range(half):
                    wide[k, :, n, i * d : (i + ONE) * d] = grads[low[ONE]][n][k * half + i, at].astype(F32)
                    wide[k, :, n, (half + i) * d : (half + i + ONE) * d] = grads[high[ONE]][n][k * half + i, at].astype(F32)

    for c in (ZERO, ONE):
        pl.when(core == c)(functools.partial(lay, c == ZERO))
    for j in range(4):
        update(j, ..., narrow[j])
    for j in range(TWO):
        for i in range(TWO * half):
            here = (slice(None), slice(None), slice(i * d, (i + ONE) * d))
            update(4 + j, here, wide[(j, *here)])
    for n in range(layers):
        for i in range(half):
            update(6, (n, slice(i * TWO * r, (i + ONE) * TWO * r)), grads[4][n][i].astype(F32))


def finish(total, grads, arrays, count):
    layers = len(grads[0])
    given = [total] + [x for some in grads for x in some] + list(arrays)
    outs = [shape(a.shape, a.dtype) for a in arrays]
    r, _, d = arrays[0].shape
    f = arrays[4].shape[2]
    return pl.pallas_call(
        functools.partial(_finish, layers=layers, count=count),
        in_specs=[IN_VMEM] * len(given),
        out_specs=[IN_VMEM] * len(outs),
        out_shape=outs,
        scratch_shapes=[pltpu.VMEM((4, r, layers, d), F32), pltpu.VMEM((2, r, layers, f), F32)],
        compiler_params=params(),
        cost_estimate=cost(10**7, *given, *outs),
        name="finish",
    )(*given)


def rotary(tokens):
    half = HEAD // 2
    angle = np.arange(tokens, dtype=np.float32)[:, None] * np.float32(THETA) ** (-np.arange(half, dtype=np.float32) / np.float32(half))
    cos, sin = np.cos(angle), np.sin(angle)
    return np.concatenate([cos, cos], 1), np.concatenate([-sin, sin], 1)


def solution(mesh):
    size = mesh.shape["dp"]
    chips = size // TWO

    def gathered(blocks):
        k, r, d = blocks.shape
        return lax.all_gather(blocks.reshape(k * r, d), "dp", axis=ZERO, tiled=True).reshape(chips, TWO * k, r, d)

    def scattered(blocks):
        _, k, r, d = blocks.shape
        return lax.psum_scatter(blocks.reshape(-ONE, d), "dp", scatter_dimension=ZERO, tiled=True).reshape(k // TWO, r, d)

    def turn(some):
        return [w.transpose(ONE, ZERO, TWO) for w in some[:6]] + [some[6]]

    def step(x, dy, *arrays):
        weights, m, v = (arrays[i : i + 7] for i in (ZERO, 7, 14))
        layers = weights[ZERO].shape[ZERO]
        h, dy = x[ZERO], dy[ZERO]
        tokens, d = h.shape
        n = weights[4].shape[TWO] // d
        per = 3 * (n // TWO)
        tables = rotary(tokens)

        own, *others = pack(turn(weights), n)
        later = [gathered(t) for t in others]
        ga = [(spread(own, size), ZERO)] + [(g, per) for g in later[:-ONE]]
        gm = [(g, ZERO) for g in later]
        kept = []
        for i in range(layers):
            q, k, v_ = project(h, ga[i], tables)
            o, lse = attend(q, k, v_)
            kept.append((h, q, k, v_, o, lse))
            if i < layers - ONE:
                h2, b, gate, up, act, h = rest(h, o, ga[i], gm[i], n)
                kept[i] += (h2, b, gate, up, act)
        pairs, inners, downs = ([None] * layers for _ in range(3))
        half = n // TWO
        for i in reversed(range(layers)):
            h, q, k, v_, o, lse, *more = kept[i]
            end = i == layers - ONE
            if end:
                b, act, dgu, dh, do, delta = rest_back(dy, h, o, ga[i], gm[i], n)
            else:
                h2, b, gate, up, act = more
                dgu, dh, do, delta = rest_back(dy, h2, o, ga[i], gm[i], n, gate, up)
                dgu, inners[i + ONE] = lax.optimization_barrier((dgu, inners[i + ONE]))
            inner, into = weights_back(b, dgu, act, dy, o, dh, gm[i][ZERO], n, end, 4 + (n if i else ZERO))
            do, inner = lax.optimization_barrier((do, inner))
            inners[i] = scattered(inner)
            if end:
                inners[i], downs[i] = inners[i][: TWO * half], inners[i][TWO * half :]
            else:
                do, pairs[i + ONE] = lax.optimization_barrier((do, pairs[i + ONE]))
            dq, dk, dv = attend_back(q, k, v_, do, lse, delta)
            if i:
                dy, into = project_back(h, dh, dq, dk, dv, tables, ga[i], into)
                both = scattered(down_back(kept[i - ONE][-ONE], dy, into, n))
                pairs[i], downs[i - ONE] = both[:TWO], both[TWO:]
            else:
                (into,) = project_back(h, None, dq, dk, dv, tables, ga[i], into)
                pairs[i] = collect(into, size)
        shared = pairs + inners
        total, *got = meet(shared + downs, len(shared), size)
        grads = [pairs, inners, got[:layers], got[layers:], downs]
        done = finish(total, grads, turn(weights) + turn(m) + turn(v), size * sum(w.size for w in weights))
        return tuple(t for i in (ZERO, 7, 14) for t in turn(done[i : i + 7]))

    states, cut = P(("rep", "dp"), None, None), P(None, "dp", None)
    return jax.shard_map(
        step,
        mesh=mesh,
        in_specs=(states, states) + (cut,) * 21,
        out_specs=(P("rep", "dp", None),) * 21,
        check_vma=False,
    )
```

```python
import functools
import math

import jax
import jax.numpy as jnp
import numpy as np
from jax import lax
from jax.experimental import pallas as pl
from jax.experimental.pallas import tpu as pltpu
from jax.sharding import PartitionSpec as P

ZERO, ONE, TWO = range(3)
HEAD = 128
LANES = 128
SUBLANES = 8
THETA = 10000
LOG2E = 1.4426950408889634
HIDDEN = -2e30
BLOCK = 512
KEYS = 256
PANEL = 1792
MIB = 2**20
F32, BF16 = jnp.float32, jnp.bfloat16
NN, NT, TN = ((1,), (0,)), ((1,), (1,)), ((0,), (0,))
IN_HBM = pl.BlockSpec(memory_space=pltpu.HBM)
IN_VMEM = pl.BlockSpec(memory_space=pltpu.VMEM)
MESH = pl.DeviceIdType.MESH


def mm(a, b, dims=NN):
    return lax.dot_general(a, b, (dims, ((), ())), preferred_element_type=F32)


def shape(dims, dtype=BF16):
    return jax.ShapeDtypeStruct(tuple(dims), dtype)


def params(vmem=60, **more):
    return pltpu.CompilerParams(vmem_limit_bytes=vmem * MIB, **more)


def cost(flops, *arrays):
    return pl.CostEstimate(flops=int(flops), transcendentals=0, bytes_accessed=sum(int(a.size) * a.dtype.itemsize for a in arrays))


def _seen(n):
    return lax.broadcasted_iota(jnp.int32, (n, n), 0) <= lax.broadcasted_iota(jnp.int32, (n, n), 1)


def _attend(q_ref, k_ref, v_ref, o_ref, lse_ref, values, *, scale):
    e = scale * LOG2E
    t, d = q_ref.shape[1:]
    values[:d, :] = v_ref[0].T
    values[d:, :] = jnp.ones((SUBLANES, t), BF16)
    seen = _seen(BLOCK)
    for a in range(0, t, BLOCK):
        n = a + BLOCK
        q = q_ref[0, a:n, :]
        s = mm(k_ref[0, :n, :], q, NT)
        parts = ([s[:a]] if a else []) + [jnp.where(seen, s[a:], HIDDEN)]
        top = functools.reduce(jnp.maximum, [s.max(0, keepdims=True) for s in parts])
        mix = mm(values[:, :n], jnp.concatenate([jnp.exp2((s - top) * e).astype(BF16) for s in parts], axis=0))
        total = mix[d : d + 1]
        o_ref[0, a:n, :] = (mix[:d] * (1 / total)).T.astype(BF16)
        lse_ref[0, :, a:n] = top * scale + jnp.log(total)


def _attend_back(q_ref, k_ref, v_ref, do_ref, lse_ref, delta_ref, dq_ref, dk_ref, dv_ref, dq, *, scale):
    e = scale * LOG2E
    t = q_ref.shape[ONE]
    seen = _seen(KEYS)
    lse, delta = lse_ref[ZERO] * LOG2E, delta_ref[ZERO]
    for a in range(ZERO, t, KEYS):
        n = a + KEYS
        k, v = k_ref[ZERO, a:n, :], v_ref[ZERO, a:n, :]
        turned = k.T
        s = mm(k, q_ref[ZERO, a:, :], NT)
        dp = mm(v, do_ref[ZERO, a:, :], NT)
        p = jnp.exp2(s * e - lse[:, a:])
        masked = jnp.where(seen, p[:, :KEYS], 0.0)
        p = jnp.concatenate([masked, p[:, KEYS:]], axis=ONE) if n < t else masked
        ds = (p * (dp - delta[:, a:])).astype(BF16)
        dv = mm(p.astype(BF16), do_ref[ZERO, a:, :])
        dk = mm(ds, q_ref[ZERO, a:, :])
        part = mm(turned, ds)
        if a:
            dq[:, a:] += part
        else:
            dq[...] = part
        dv_ref[ZERO, a:n, :] = dv.astype(BF16)
        dk_ref[ZERO, a:n, :] = (dk * scale).astype(BF16)
        dq_ref[ZERO, a:n, :] = (dq[:, a:n] * scale).T.astype(BF16)


def one_head(q, rows_of=None):
    dims = (1, *q.shape[1:]) if rows_of is None else (1, 1, q.shape[1])
    return pl.BlockSpec(dims, lambda i: (i, 0, 0))


def attend(q, k, v):
    n, t, d = q.shape
    spec, stat = one_head(q), one_head(q, True)
    return pl.pallas_call(
        functools.partial(_attend, scale=d**-0.5),
        grid=(n,),
        in_specs=[spec] * 3,
        out_specs=[spec, stat],
        out_shape=[shape(q.shape), shape((n, 1, t), F32)],
        scratch_shapes=[pltpu.VMEM((d + SUBLANES, t), BF16)],
        compiler_params=params(),
        cost_estimate=cost(4 * n * t * t * d, q, k, v, q),
        name="attend",
    )(q, k, v)


def attend_back(q, k, v, do, lse, delta):
    n, t, d = q.shape
    spec, stat = one_head(q), one_head(q, True)
    return pl.pallas_call(
        functools.partial(_attend_back, scale=d**-0.5),
        grid=(n,),
        in_specs=[spec] * 4 + [stat] * 2,
        out_specs=[spec] * 3,
        out_shape=[shape(q.shape)] * 3,
        scratch_shapes=[pltpu.VMEM((d, t), F32)],
        compiler_params=params(),
        cost_estimate=cost(10 * n * t * t * d, q, k, v, do, q, k, v),
        name="attend_back",
    )(q, k, v, do, lse, delta)


def flat(x):
    return x.reshape(-1, x.shape[-1])


def norm_parts(h):
    wide = h.astype(F32)
    return wide, lax.rsqrt(jnp.mean(wide * wide, -1, keepdims=True) + 1e-6)


def norm_back(by_a, wide, scale):
    by_a = by_a.astype(F32)
    dot = jnp.sum(by_a * wide, -1, keepdims=True)
    return by_a * scale - wide * (scale * scale * scale * (1 / wide.shape[-1]) * dot)


def joined(ref):
    return jnp.concatenate([ref[i] for i in range(ref.shape[0])], axis=1)


def rows(tile, width):
    return pl.BlockSpec((tile, width), lambda i: (i, 0))


def heads_of(n, tile):
    return pl.BlockSpec((n, tile, HEAD), lambda i: (0, i, 0))


def number(g, first, i):
    many, at = i
    return at // many * (g.shape[1] // 2) + first + at % many


def load(g, first, name, ref, n, sems):
    d, half = g.shape[3], n // TWO
    if name == "qkv":
        return [[pltpu.make_async_copy(g.at[:, number(g, first, (TWO, i))], ref.at[:, :, i * d : (i + ONE) * d], sems[ZERO]) for i in range(3)]]
    if name == "wo":
        return [[pltpu.make_async_copy(g.at[:, number(g, first, (TWO, 3))], ref, sems[ZERO])]]
    if name == "w_down":
        at = [(i, number(g, first + TWO * half, (half, i))) for i in (ZERO, half)]
        some = g.shape[ZERO] // TWO
        return [[pltpu.make_async_copy(g.at[pl.ds(c, some), pl.ds(b, half)], ref.at[pl.ds(c, some), pl.ds(i, half)], sem) for i, b in at]
                for c, sem in zip((ZERO, some), sems)]
    first += half if name == "w_up" else ZERO
    return [[pltpu.make_async_copy(g.at[:, number(g, first, (half, i))], ref.at[k, :, :, i % half * d : (i % half + ONE) * d], sem) for i in range(k * half, (k + ONE) * half)]
            for k, sem in enumerate(sems)]


def at_first(groups, steps=1):
    first = pl.program_id(0) == 0
    begin = first if steps == 1 else first & (pl.program_id(1) == 0)

    @pl.when(begin)
    def _():
        for group in groups:
            for c in group:
                c.start()

    def ready(k):
        @pl.when(begin if steps == 1 or not k else first & (pl.program_id(1) == k - 1))
        def _():
            for c in groups[k]:
                c.wait()

    return ready


def inner_weights(g_refs, firsts, refs, n, sem, steps=1):
    wo, *inner = refs
    sems = sem.at[0], sem.at[1]
    halves = zip(*[load(g_refs[1], firsts[1], name, ref, n, sems) for name, ref in zip(("w_gate", "w_up", "w_down"), inner)])
    return at_first(load(g_refs[0], firsts[0], "wo", wo, n, [sem.at[2]]) + [sum(half, []) for half in halves], steps)


def inner_scratch(g, n):
    chips, _, r, d = g.shape
    return [pltpu.VMEM((chips, r, d), BF16), pltpu.VMEM((2, chips, r, n // 2 * d), BF16), pltpu.VMEM((2, chips, r, n // 2 * d), BF16), pltpu.VMEM((chips, n, r, d), BF16),
            pltpu.SemaphoreType.DMA((3,))]


def _project(h_ref, cos_ref, sin_ref, g_ref, q_ref, k_ref, v_ref, w, sem, *, first):
    at_first(load(g_ref, first, "qkv", w, ZERO, [sem.at[ZERO]]))(ZERO)
    d = h_ref.shape[ONE]
    wide, scale = norm_parts(h_ref[...])
    t = mm((wide * scale).astype(BF16), flat(w[...])).astype(BF16)
    cos, sin = cos_ref[...], sin_ref[...]
    for n, ref in enumerate((q_ref, k_ref, v_ref)):
        for i in range(ref.shape[ZERO]):
            x = t[:, n * d + i * HEAD : n * d + (i + ONE) * HEAD]
            if n < TWO:
                x = x.astype(F32)
                x = (x * cos + pltpu.roll(x, HEAD // TWO, ONE) * sin).astype(BF16)
            ref[i] = x


def project(h, ga, tables, tile=512):
    g, first = ga, 0
    tokens, d = h.shape
    chips, _, r, _ = g.shape
    n = d // HEAD
    out = shape((n, tokens, HEAD))
    return pl.pallas_call(
        functools.partial(_project, first=first),
        grid=(tokens // tile,),
        in_specs=[rows(tile, d), rows(tile, HEAD), rows(tile, HEAD), IN_HBM],
        out_specs=[heads_of(n, tile)] * 3,
        out_shape=[out] * 3,
        scratch_shapes=[pltpu.VMEM((chips, r, 3 * d), BF16), pltpu.SemaphoreType.DMA((1,))],
        compiler_params=params(),
        cost_estimate=cost(6 * tokens * d * d, h, out, out, out),
        name="project",
    )(h, *tables, g)


def _rest(h_ref, o_ref, ga_ref, gm_ref, h2_ref, b_ref, gate_ref, up_ref, act_ref, y_ref, wo, wg, wu, wd, sem, *, firsts):
    ready = inner_weights((ga_ref, gm_ref), firsts, (wo, wg, wu, wd), wd.shape[ONE], sem)
    ready(ZERO)
    h2 = h_ref[...] + mm(joined(o_ref), flat(wo[...])).astype(BF16)
    h2_ref[...] = h2
    wide, scale = norm_parts(h2)
    b = (wide * scale).astype(BF16)
    b_ref[...] = b
    total = 0.0
    w_down = lambda a: flat(wd[a // PANEL * (wd.shape[ZERO] // TWO) : (a // PANEL + ONE) * (wd.shape[ZERO] // TWO)])
    for a in range(ZERO, gate_ref.shape[ONE], PANEL):
        ready(ONE + a // PANEL)
        here = slice(a, a + PANEL)
        gate = mm(b, flat(wg[a // PANEL]))
        up = mm(b, flat(wu[a // PANEL]))
        gate_ref[:, here] = gate
        up_ref[:, here] = up
        act = (gate * jax.nn.sigmoid(gate) * up).astype(BF16)
        act_ref[:, here] = act
        total += mm(act, w_down(a))
    y_ref[...] = h2 + total.astype(BF16)


def rest(h, o, ga, gm, n, tile=256):
    tokens, d = h.shape
    f = n * d
    assert f == 2 * PANEL
    narrow = shape((tokens, d))
    return pl.pallas_call(
        functools.partial(_rest, firsts=(0, 0)),
        grid=(tokens // tile,),
        in_specs=[rows(tile, d), heads_of(d // HEAD, tile), IN_HBM, IN_HBM],
        out_specs=[rows(tile, d)] * 2 + [rows(tile, f)] * 3 + [rows(tile, d)],
        out_shape=[narrow, narrow, shape((tokens, f), F32), shape((tokens, f), F32), shape((tokens, f)), narrow],
        scratch_shapes=inner_scratch(gm, n),
        compiler_params=params(),
        cost_estimate=cost(2 * tokens * d * (d + 3 * f), h, o, gm),
        name="rest",
    )(h, o, ga, gm)


def hidden_back(d_act, gate, up):
    d_act = d_act.astype(BF16).astype(F32)
    sig = jax.nn.sigmoid(gate)
    silu = gate * sig
    return (silu * up).astype(BF16), (d_act * up * (sig + silu * (1 - sig))).astype(BF16), (d_act * silu).astype(BF16)


def to_attention(dh, o_ref, wo, do_ref, delta_ref):
    do = mm(dh, flat(wo[...]), NT).astype(BF16)
    for i in range(do_ref.shape[0]):
        part = do[:, i * HEAD : (i + 1) * HEAD]
        do_ref[i] = part
        delta_ref[i] = jnp.sum((part.astype(F32) * o_ref[i].astype(F32)).T, axis=0, keepdims=True)


def _rest_back(dy_ref, h_ref, o_ref, gate_ref, up_ref, ga_ref, gm_ref, dgu_ref, dh_ref, do_ref, delta_ref, wo, wg, wu, wd, sem, *, firsts):
    ready = inner_weights((ga_ref, gm_ref), firsts, (wo, wg, wu, wd), wd.shape[ONE], sem)
    ready(ZERO)
    dy = dy_ref[...]
    wide, scale = norm_parts(h_ref[...])
    total = 0.0
    some = wd.shape[ZERO] // TWO
    for k in range(TWO):
        ready(ONE + k)
        here = slice(k * PANEL, (k + ONE) * PANEL)
        d_act = mm(dy, flat(wd[k * some : (k + ONE) * some]), NT)
        _, d_gate, d_up = hidden_back(d_act, gate_ref[:, here], up_ref[:, here])
        dgu_ref[ZERO, :, here] = d_gate
        dgu_ref[ONE, :, here] = d_up
        total += mm(d_gate, flat(wg[k]), NT) + mm(d_up, flat(wu[k]), NT)
    dh = dy + norm_back(total.astype(BF16), wide, scale).astype(BF16)
    dh_ref[...] = dh
    to_attention(dh, o_ref, wo, do_ref, delta_ref)


def rest_back(dy, h, o, ga, gm, n, gate, up, tile=256):
    tokens, d = dy.shape
    f = n * d
    heads = d // HEAD
    given = [dy, h, o, gate, up, ga, gm]
    return pl.pallas_call(
        functools.partial(_rest_back, firsts=(ZERO, ZERO)),
        grid=(tokens // tile,),
        in_specs=[rows(tile, d), rows(tile, d), heads_of(heads, tile)] + [rows(tile, f)] * TWO + [IN_HBM, IN_HBM],
        out_specs=[pl.BlockSpec((TWO, tile, f), lambda i: (ZERO, i, ZERO)), rows(tile, d), heads_of(heads, tile), pl.BlockSpec((heads, ONE, tile), lambda i: (ZERO, ZERO, i))],
        out_shape=[shape((TWO, tokens, f)), shape((tokens, d)), shape((heads, tokens, HEAD)), shape((heads, ONE, tokens), F32)],
        scratch_shapes=inner_scratch(gm, n),
        compiler_params=params(),
        cost_estimate=cost(TWO * tokens * d * (d + 3 * f), *given),
        name="rest_back",
    )(*given)


def _rest_last(dy_ref, h_ref, o_ref, ga_ref, gm_ref, b_ref, act_ref, dgu_ref, dh_ref, do_ref, delta_ref, wo, wg, wu, wd, sem, h2, total, *, firsts):
    ready = inner_weights((ga_ref, gm_ref), firsts, (wo, wg, wu, wd), wd.shape[ONE], sem, TWO)
    k = pl.program_id(ONE)
    ready(ZERO)

    @pl.when(k == ZERO)
    def _():
        h2[...] = h_ref[...] + mm(joined(o_ref), flat(wo[...])).astype(BF16)
        wide, scale = norm_parts(h2[...])
        b_ref[...] = (wide * scale).astype(BF16)
        total[...] = jnp.zeros_like(total)

    ready(ONE)
    ready(TWO)
    some = wd.shape[ZERO] // TWO
    b = b_ref[...]
    gate, up = mm(b, flat(wg[k])), mm(b, flat(wu[k]))
    d_act = mm(dy_ref[...], flat(wd[pl.ds(k * some, some)]), NT)
    act_ref[...], d_gate, d_up = hidden_back(d_act, gate, up)
    dgu_ref[ZERO] = d_gate
    dgu_ref[ONE] = d_up
    total[...] += mm(d_gate, flat(wg[k]), NT) + mm(d_up, flat(wu[k]), NT)

    @pl.when(k == ONE)
    def _():
        wide, scale = norm_parts(h2[...])
        dh = dy_ref[...] + norm_back(total[...].astype(BF16), wide, scale).astype(BF16)
        dh_ref[...] = dh
        to_attention(dh, o_ref, wo, do_ref, delta_ref)


def rest_last(dy, h, o, ga, gm, n, tile=512):
    tokens, d = dy.shape
    f = n * d
    heads = d // HEAD
    given = [dy, h, o, ga, gm]
    tall = pl.BlockSpec((tile, d), lambda i, k: (i, ZERO))
    split = pl.BlockSpec((heads, tile, HEAD), lambda i, k: (ZERO, i, ZERO))
    return pl.pallas_call(
        functools.partial(_rest_last, firsts=(ZERO, ZERO)),
        grid=(tokens // tile, TWO),
        in_specs=[tall, tall, split, IN_HBM, IN_HBM],
        out_specs=[tall, pl.BlockSpec((tile, f // TWO), lambda i, k: (i, k)), pl.BlockSpec((TWO, tile, f // TWO), lambda i, k: (ZERO, i, k)), tall, split,
                   pl.BlockSpec((heads, ONE, tile), lambda i, k: (ZERO, ZERO, i))],
        out_shape=[shape((tokens, d)), shape((tokens, f)), shape((TWO, tokens, f)), shape((tokens, d)), shape((heads, tokens, HEAD)),
                   shape((heads, ONE, tokens), F32)],
        scratch_shapes=inner_scratch(gm, n) + [pltpu.VMEM((tile, d), BF16), pltpu.VMEM((tile, d), F32)],
        compiler_params=params(63),
        cost_estimate=cost(TWO * tokens * d * (TWO * d + 5 * f), *given),
        name="rest_last",
    )(*given)


def _weights_back(b_hbm, dgu_hbm, act_hbm, dy_hbm, o_hbm, dh_hbm, out_ref, out2_ref, b, bt, stage, dgu, act, dy, o, dh, sem, in_sem, *, panels):
    s = pl.program_id(ZERO)
    chips, blocks, r, d = out_ref.shape
    n = panels
    half = n // TWO
    per = blocks // TWO
    downs = n if per > TWO * half else ZERO
    early = 4
    width = dgu.shape[TWO]
    wides = [pltpu.make_async_copy(dgu_hbm.at[k // TWO, :, pl.ds(k % TWO * width, width)], dgu.at[k % TWO], in_sem.at[5 + k % TWO]) for k in range(early)]
    b_load = pltpu.make_async_copy(b_hbm, b, in_sem.at[7])
    late = [pltpu.make_async_copy(a, b, in_sem.at[i]) for i, (a, b) in enumerate(((o_hbm, o), (dh_hbm, dh)) + (((dy_hbm, dy),) if downs else ()))]
    acts = [pltpu.make_async_copy(act_hbm.at[:, pl.ds(k * d, d)], act.at[k % TWO], in_sem.at[3 + k % TWO]) for k in range(downs)]

    def gate_up(k):
        which, core = divmod(k, TWO)
        return [pltpu.make_async_copy(stage.at[k % TWO, :, :, pl.ds(i * d, d)], out_ref.at[:, core * per + which * half + i], sem.at[k % TWO]) for i in range(half)]

    def down(k):
        some = chips // n
        src = stage.at[k % TWO, :, :, pl.ds(ZERO, d)]
        return [pltpu.make_async_copy(src.at[pl.ds(i * n + j, ONE)], out_ref.at[pl.ds(k * some + i, ONE), j // half * per + TWO * half + j % half], sem.at[k % TWO])
                for i in range(some) for j in range(n)]

    steps = [gate_up(k) for k in range(early)] + [down(k) for k in range(downs)]
    last = early + downs
    steps.append([pltpu.make_async_copy(stage.at[ZERO, :, :, pl.ds(ZERO, d)], out2_ref.at[:, out2_ref.shape[ONE] // TWO + ONE], sem.at[ZERO])])
    for k in range(len(steps)):
        @pl.when(s == k)
        def _(k=k):
            if k == ZERO:
                b_load.start()
                wides[ZERO].start()
                b_load.wait()
                bt[...] = b[...].T
            if k < early:
                wides[k].wait()
            if k + ONE < early:
                wides[k + ONE].start()
            if k == ZERO:
                for c in late:
                    c.start()
            if k >= TWO:
                for c in steps[k - TWO]:
                    c.wait()
            if early - ONE <= k < last - ONE:
                acts[k - early + ONE].start()
            if k == early and downs:
                late[TWO].wait()
            if early <= k < last:
                acts[k - early].wait()
            if k == last:
                late[ZERO].wait()
                late[ONE].wait()

    @pl.when(s < early)
    def _():
        stage[lax.rem(s, TWO)] = mm(bt[...], dgu[lax.rem(s, TWO)]).astype(BF16).reshape(chips, r, half * d)

    if downs:
        @pl.when((s >= early) & (s < last))
        def _():
            stage[lax.rem(s, TWO), :, :, :d] = mm(act[lax.rem(s, TWO)], dy[...], TN).astype(BF16).reshape(chips, r, d)

    @pl.when(s == last)
    def _():
        stage[ZERO, :, :, :d] = mm(joined(o), dh[...], TN).astype(BF16).reshape(chips, r, d)

    for k in range(len(steps)):
        @pl.when(s == k)
        def _(k=k):
            for c in steps[k]:
                c.start()
            if k == len(steps) - ONE:
                for c in steps[k - ONE] + steps[k]:
                    c.wait()


def weights_back(b, dgu, act, dy, o, dh, g, n, down, others):
    tokens, d = b.shape
    chips, _, r, _ = g.shape
    f = n * d
    panel = f // TWO
    return pl.pallas_call(
        functools.partial(_weights_back, panels=n),
        grid=(4 + (n if down else ZERO) + ONE,),
        in_specs=[IN_HBM] * 6,
        out_specs=[IN_HBM, IN_HBM],
        out_shape=[shape((chips, (3 if down else TWO) * n, r, d)), shape((chips, others, r, d))],
        scratch_shapes=[pltpu.VMEM((tokens, d), BF16), pltpu.VMEM((d, tokens), BF16), pltpu.VMEM((TWO, chips, r, panel), BF16),
                        pltpu.VMEM((TWO, tokens, panel), BF16), pltpu.VMEM((TWO, tokens, d), BF16), pltpu.VMEM((tokens, d), BF16),
                        pltpu.VMEM(o.shape, BF16), pltpu.VMEM((tokens, d), BF16), pltpu.SemaphoreType.DMA((TWO,)), pltpu.SemaphoreType.DMA((8,))],
        compiler_params=params(),
        cost_estimate=cost(TWO * tokens * d * (d + (3 if down else TWO) * f), b, dgu, act, dy),
        name="weights_back" if down else "weights_back_some",
    )(b, dgu, act, dy, o, dh)


def _down_back(act_ref, dy_ref, _, out_ref, stage, sem, *, panels):
    k = pl.program_id(0)
    chips, blocks, r, d = out_ref.shape
    some, half = chips // panels, panels // 2

    def copies(k):
        return [pltpu.make_async_copy(stage.at[k % 2, pl.ds(i * panels + j, 1)], out_ref.at[pl.ds(k * some + i, 1), j // half * (blocks // 2) + 2 + j % half], sem.at[k % 2])
                for i in range(some) for j in range(panels)]

    for a in range(2, panels):
        @pl.when(k == a)
        def _(a=a):
            for c in copies(a - 2):
                c.wait()

    stage[lax.rem(k, 2)] = mm(act_ref[...], dy_ref[...], TN).astype(BF16).reshape(chips, r, d)
    for a in range(panels):
        @pl.when(k == a)
        def _(a=a):
            for c in copies(a):
                c.start()
            if a == panels - 1:
                for c in copies(a - 1) + copies(a):
                    c.wait()


def down_back(act, dy, into, n):
    tokens, d = dy.shape
    chips, _, r, _ = into.shape
    return pl.pallas_call(
        functools.partial(_down_back, panels=n),
        grid=(n,),
        in_specs=[pl.BlockSpec((tokens, d), lambda s: (0, s)), pl.BlockSpec((tokens, d), lambda s: (0, 0), pipeline_mode=pl.Buffered(1)), IN_HBM],
        out_specs=IN_HBM,
        out_shape=shape(into.shape),
        scratch_shapes=[pltpu.VMEM((2, chips, r, d), BF16), pltpu.SemaphoreType.DMA((2,))],
        input_output_aliases={2: 0},
        compiler_params=params(),
        cost_estimate=cost(2 * tokens * d * n * d, act, dy),
        name="down_back",
    )(act, dy, into)


def _project_back(*refs, last, first):
    if last:
        h_ref, dq_ref, dk_ref, dv_ref, cos_ref, sin_ref, _, out_ref, total, stage, sem = refs
    else:
        h_ref, dh_ref, dq_ref, dk_ref, dv_ref, cos_ref, sin_ref, g_ref, _, dx_ref, out_ref, total, stage, sem, w, wsem = refs
        ready = at_first(load(g_ref, first, "qkv", w, ZERO, [wsem.at[ZERO]]))
    s = pl.program_id(ZERO)
    chips, blocks, r, d = out_ref.shape

    @pl.when(s == ZERO)
    def _():
        total[...] = jnp.zeros_like(total)

    wide, scale = norm_parts(h_ref[...])
    a = (wide * scale).astype(BF16)
    cos, sin = cos_ref[...], sin_ref[...]
    def back(ref):
        x = ref.astype(F32)
        return (x * cos - pltpu.roll(x, HEAD // TWO, ONE) * sin).astype(BF16)

    parts = [[dv_ref[i] for i in range(dv_ref.shape[ZERO])]] + [[back(ref[i]) for i in range(ref.shape[ZERO])] for ref in (dq_ref, dk_ref)]
    parts = [jnp.concatenate(p, axis=ONE) for p in parts[ONE:] + parts[:ONE]]
    if last:
        for i in (TWO, ZERO, ONE):
            total[:, i * d : (i + ONE) * d] += mm(a, parts[i], TN)
    else:
        t = jnp.concatenate(parts, axis=ONE)
        total[...] += mm(a, t, TN)
        ready(ZERO)
        by_a = mm(t, flat(w[...]), NT)
        dx_ref[...] = dh_ref[...] + norm_back(by_a.astype(BF16), wide, scale).astype(BF16)

    @pl.when(s == pl.num_programs(ZERO) - ONE)
    def _():
        done = [pltpu.make_async_copy(stage.at[:, :, pl.ds(i * d, d)], out_ref.at[:, i // TWO * (blocks // TWO) + i % TWO], sem.at[i]) for i in range(3)]
        for i in range(3):
            stage[:, :, i * d : (i + ONE) * d] = total[:, i * d : (i + ONE) * d].astype(BF16).reshape(chips, r, d)
            done[i].start()
        for c in done:
            c.wait()


def project_back(h, dh, dq, dk, dv, tables, ga, into, tile=512):
    tokens, d = h.shape
    n = d // HEAD
    last = dh is None
    chips, _, r, _ = into.shape
    given = [h] + ([] if last else [dh]) + [dq, dk, dv, *tables] + ([] if last else [ga]) + [into]
    specs = [rows(tile, d)] * (ONE if last else TWO) + [heads_of(n, tile)] * 3 + [rows(tile, HEAD)] * TWO + [IN_HBM] * (ONE if last else TWO)
    outs = ([] if last else [(rows(tile, d), shape((tokens, d)))]) + [(IN_HBM, shape(into.shape))]
    blocks = pltpu.VMEM((chips, r, 3 * d), BF16)
    scratch = [pltpu.VMEM((d, 3 * d), F32), blocks, pltpu.SemaphoreType.DMA((3,))] + ([] if last else [blocks, pltpu.SemaphoreType.DMA((ONE,))])
    return pl.pallas_call(
        functools.partial(_project_back, last=last, first=ZERO),
        grid=(tokens // tile,),
        in_specs=specs,
        out_specs=[s for s, _ in outs],
        out_shape=[s for _, s in outs],
        scratch_shapes=scratch,
        input_output_aliases={len(given) - ONE: len(outs) - ONE},
        compiler_params=params(),
        cost_estimate=cost((ONE if last else TWO) * 6 * tokens * d * d, h, dq, dk, dv),
        name="project_back_last" if last else "project_back",
    )(*given)


class Place:
    def __init__(self, size):
        self.chips = size // 2
        self.side = math.isqrt(self.chips)
        me = lax.axis_index("dp")
        self.core = lax.rem(me, 2)
        chip = lax.div(me, 2)
        self.x, self.y = lax.div(chip, self.side), lax.rem(chip, self.side)
        self.other = dict(device_id={"dp": me + 1 - 2 * self.core}, device_id_type=MESH)

    def at(self, u, i, j):
        dx, dy = (j, i) if u else (i, j)
        wrap = lambda a: lax.rem(a + self.side, self.side)
        return wrap(self.x + dx) * self.side + wrap(self.y + dy)

    def to(self, u, i, j):
        return dict(device_id={"dp": self.at(u, i, j) * 2 + self.core}, device_id_type=MESH)

    def greet(self):
        barrier = pltpu.get_barrier_semaphore()
        peers = [self.other] + [self.to(0, i, j) for i, j in ((1, 0), (-1, 0), (0, 1), (0, -1))]
        for peer in peers:
            pl.semaphore_signal(barrier, inc=1, **peer)
        pl.semaphore_wait(barrier, len(peers))


CUT = 32


def _spread(own_ref, out_ref, out_sem, in_sem, over_out, over_in, own_sem, *, size):
    here = Place(size)
    far, back = here.side // TWO, here.side - ONE
    r = own_ref.shape[ONE]
    parts = (slice(ZERO, r), slice(ZERO, CUT), slice(CUT, r))
    keys = [(u, *k) for u in (ZERO, ONE) for k in
            [(ONE, ZERO, ZERO), (back, ZERO, ZERO), (far, ZERO, ONE), (far, ZERO, TWO)] + [(i, j, p) for i in range(here.side) for j, p in ((ONE, ZERO), (back, ZERO), (far, ONE), (far, TWO))]]

    def slot(u, i, j, p):
        return out_ref.at[here.at(u, -i, -j), here.core * TWO + u, parts[p]]

    started = []

    def send(u, i, j, p, step, key):
        k = keys.index((u, *key))
        src = own_ref.at[u] if (i, j) == (ZERO, ZERO) else slot(u, i, j, p)
        copy = pltpu.make_async_remote_copy(src, slot(u, i, j, p), out_sem.at[k], in_sem.at[k], **here.to(u, *step))
        copy.start()
        started.append(copy)

    def wait(u, *key):
        k = keys.index((u, *key))
        ref = slot(u, *key)
        pltpu.make_async_remote_copy(ref, ref, out_sem.at[k], in_sem.at[k], **here.to(u, ONE, ZERO)).wait_recv()

    def over(u, i, j):
        k = u * here.chips + i * here.side + j
        src = own_ref.at[u] if (i, j) == (ZERO, ZERO) else slot(u, i, j, ZERO)
        copy = pltpu.make_async_remote_copy(src, slot(u, i, j, ZERO), over_out.at[k], over_in.at[k], **here.other)
        copy.start()
        started.append(copy)

    def fan(u, i):
        send(u, i, ZERO, ZERO, (ZERO, ONE), (i, ONE, ZERO))
        send(u, i, ZERO, ZERO, (ZERO, -ONE), (i, back, ZERO))

    def second(u, i):
        wait(u, i, ONE, ZERO)
        send(u, i, ONE, ONE, (ZERO, ONE), (i, far, ONE))
        wait(u, i, back, ZERO)
        send(u, i, back, TWO, (ZERO, -ONE), (i, far, TWO))
        over(u, i, ONE)
        over(u, i, back)

    here.greet()
    for u in (ZERO, ONE):
        send(u, ZERO, ZERO, ZERO, (ONE, ZERO), (ONE, ZERO, ZERO))
        send(u, ZERO, ZERO, ZERO, (-ONE, ZERO), (back, ZERO, ZERO))
        fan(u, ZERO)
    mine = [pltpu.make_async_copy(own_ref.at[u], slot(u, ZERO, ZERO, ZERO), own_sem.at[u]) for u in (ZERO, ONE)]
    for u in (ZERO, ONE):
        over(u, ZERO, ZERO)
        mine[u].start()
    for u in (ZERO, ONE):
        wait(u, ONE, ZERO, ZERO)
        send(u, ONE, ZERO, ONE, (ONE, ZERO), (far, ZERO, ONE))
        fan(u, ONE)
        wait(u, back, ZERO, ZERO)
        send(u, back, ZERO, TWO, (-ONE, ZERO), (far, ZERO, TWO))
        fan(u, back)
    for u in (ZERO, ONE):
        over(u, ONE, ZERO)
        over(u, back, ZERO)
        second(u, ZERO)
    for u in (ZERO, ONE):
        wait(u, far, ZERO, ONE)
        wait(u, far, ZERO, TWO)
        fan(u, far)
        over(u, far, ZERO)
    for i in (ONE, back, far):
        for u in (ZERO, ONE):
            second(u, i)
    for i in (ZERO, ONE, back, far):
        for u in (ZERO, ONE):
            wait(u, i, far, ONE)
            wait(u, i, far, TWO)
            over(u, i, far)
    for c in mine:
        c.wait()
    for u in (ZERO, ONE):
        for k in range(here.chips):
            ref = out_ref.at[here.at(u, -(k // here.side), -(k % here.side)), (ONE - here.core) * TWO + u]
            pltpu.make_async_remote_copy(ref, ref, over_out.at[u * here.chips + k], over_in.at[u * here.chips + k], **here.other).wait_recv()
    for c in started:
        c.wait_send()


def spread(own, size):
    messages = 2 * (math.isqrt(size // 2) + 1) * 4
    dma = pltpu.SemaphoreType.DMA
    return pl.pallas_call(
        functools.partial(_spread, size=size),
        in_specs=[IN_HBM],
        out_specs=IN_HBM,
        out_shape=shape((size // 2, 4, *own.shape[1:])),
        scratch_shapes=[dma((messages,)), dma((messages,)), dma((size,)), dma((size,)), dma((2,))],
        compiler_params=params(60, collective_id=3, has_side_effects=True),
        cost_estimate=pl.CostEstimate(flops=10**10, transcendentals=0, bytes_accessed=10**7),
        name="spread",
    )(own)


def _collect(grads_ref, out_ref, own, sib, total, far_out, far_in, near_out, near_in, over_out, over_in, far_sem, near_sem, own_sem, *, size):
    here = Place(size)
    far, back = here.side // TWO, here.side - ONE
    r = grads_ref.shape[TWO]
    parts = ((slice(ZERO, CUT), (ZERO, ONE)), (slice(CUT, r), (ZERO, -ONE)))
    order = (far, ONE, back, ZERO)
    both = [(u, i) for i in order for u in (ZERO, ONE)]
    started, waiting = [], []

    def start(copies):
        flush()
        waiting.extend(copies)

    def flush():
        for c in waiting:
            c.start()
        started.extend(waiting)
        waiting.clear()

    mine = pltpu.make_async_copy(grads_ref.at[:, pl.ds(TWO * here.core, TWO)], own, own_sem)
    mine.start()
    here.greet()
    overs = {}
    for j in (far, ONE, back, ZERO):
        for u, i in both:
            k = u * here.chips + i * here.side + j
            overs[u, i, j] = pltpu.make_async_remote_copy(grads_ref.at[here.at(u, i, j), TWO * (ONE - here.core) + u], sib.at[k], over_out.at[k], over_in.at[k],
                                                          **here.other)
            overs[u, i, j].start()
    mine.wait()

    def ours(u, i, j):
        overs[u, i, j].wait_recv()
        return own[here.at(u, i, j), u].astype(F32) + sib[u * here.chips + i * here.side + j].astype(F32)

    def turn(u, i, step):
        return step if i < here.side else step[::-ONE]

    def first(u, i, block):
        far_out[u, i] = block.astype(BF16)
        start([pltpu.make_async_remote_copy(far_out.at[u, i, rows_], far_in.at[u, i, rows_], far_sem.at[ZERO, u, i, n], far_sem.at[ONE, u, i, n],
                                            **here.to(u, *turn(u, i, step))) for n, (rows_, step) in enumerate(parts)])

    def landed(sems, ref, u, i, n):
        pltpu.make_async_remote_copy(ref, ref, sems.at[ZERO, u, i, n], sems.at[ONE, u, i, n], **here.other).wait_recv()

    def second(u, i, block, n):
        rows_, step = parts[n]
        landed(far_sem, far_in.at[u, i, rows_], u, i, n)
        pieces = [block[:CUT], block[CUT:]]
        pieces[n] += far_in[u, i, rows_].astype(F32)
        near_out[u, i, n, :CUT] = pieces[ZERO].astype(BF16)
        near_out[u, i, n, CUT:] = pieces[ONE].astype(BF16)
        start([pltpu.make_async_remote_copy(near_out.at[u, i, n], near_in.at[u, i, n], near_sem.at[ZERO, u, i, n], near_sem.at[ONE, u, i, n],
                                            **here.to(u, *turn(u, i, step)))])

    def third(u, i, block):
        for n in (ZERO, ONE):
            landed(near_sem, near_in.at[u, i, n], u, i, n)
            block += near_in[u, i, n].astype(F32)
        return block

    for u, i in both:
        first(u, i, ours(u, i, far))
    for u, i in both:
        for n, j in enumerate((ONE, back)):
            second(u, i, ours(u, i, j), n)
    for u, i in both:
        block = third(u, i, ours(u, i, ZERO))
        if i == far:
            first(u, here.side, block)
        elif i:
            second(u, here.side, block, ZERO if i == ONE else ONE)
        else:
            total[u] = block
    flush()
    for u in (ZERO, ONE):
        out_ref[u] = third(u, here.side, total[u]).astype(BF16)
    for c in list(overs.values()) + started:
        c.wait_send()


def collect(grads, size):
    chips, _, r, d = grads.shape
    rings = math.isqrt(chips) + ONE
    dma, vmem = pltpu.SemaphoreType.DMA, pltpu.VMEM
    return pl.pallas_call(
        functools.partial(_collect, size=size),
        in_specs=[IN_HBM],
        out_specs=IN_VMEM,
        out_shape=shape((TWO, r, d)),
        scratch_shapes=[vmem((chips, TWO, r, d), BF16), vmem((size, r, d), BF16), vmem((TWO, r, d), F32), vmem((TWO, rings, r, d), BF16), vmem((TWO, rings, r, d), BF16),
                        vmem((TWO, rings, TWO, r, d), BF16), vmem((TWO, rings, TWO, r, d), BF16), dma((size,)), dma((size,)), dma((TWO, TWO, rings, TWO)),
                        dma((TWO, TWO, rings, TWO)), dma],
        compiler_params=params(60, collective_id=4, has_side_effects=True),
        cost_estimate=pl.CostEstimate(flops=10**10, transcendentals=ZERO, bytes_accessed=10**7),
        name="collect",
    )(grads)


def _pack(*refs, layer, n):
    given, outs, weights, (send, got, send_sem, got_sem, sem) = refs[:7], refs[7:9], refs[9:16], refs[16:]
    loads = [pltpu.make_async_copy(a, b, sem.at[i]) for i, (a, b) in enumerate(zip(given, weights))]
    for c in loads:
        c.start()
    me = lax.axis_index("dp")
    core = lax.rem(me, TWO)
    other = dict(device_id={"dp": me + ONE - TWO * core}, device_id_type=MESH)
    half = n // TWO
    r, _, d = weights[ZERO].shape
    shared = TWO + TWO * half
    barrier = pltpu.get_barrier_semaphore()
    pl.semaphore_signal(barrier, inc=ONE, **other)

    def part(k, core):
        if k < TWO:
            return weights[TWO * core + k][...].astype(F32)[:, layer].astype(BF16)
        which, i = divmod(k - TWO, half)
        i += core * half
        return weights[4 + which][:, :, i * d : (i + ONE) * d].astype(F32)[:, layer].astype(BF16)

    def into(k):
        return (outs[ZERO], k) if k < TWO else (outs[ONE], k - TWO)

    def give(core):
        for k in range(shared):
            send[k] = part(k, ONE - core)

    def keep(core):
        for k in range(shared):
            out, at = into(k)
            out[at, core * r : (core + ONE) * r] = part(k, core)

    def take(core):
        for k in range(shared):
            out, at = into(k)
            out[at, (ONE - core) * r : (TWO - core) * r] = got[k]

    for c in loads:
        c.wait()
    for c in (ZERO, ONE):
        pl.when(core == c)(functools.partial(give, c))
    pl.semaphore_wait(barrier, ONE)
    copy = pltpu.make_async_remote_copy(send, got, send_sem, got_sem, **other)
    copy.start()
    for c in (ZERO, ONE):
        pl.when(core == c)(functools.partial(keep, c))
    for i in range(half):
        outs[ONE][TWO * half + i] = weights[6][layer, i * TWO * r : (i + ONE) * TWO * r]
    copy.wait()
    for c in (ZERO, ONE):
        pl.when(core == c)(functools.partial(take, c))


def pack(weights, n, layer):
    r, _, d = weights[ZERO].shape
    half = n // TWO
    return pl.pallas_call(
        functools.partial(_pack, layer=layer, n=n),
        in_specs=[IN_HBM] * 7,
        out_specs=[IN_VMEM] * TWO,
        out_shape=[shape((k, TWO * r, d)) for k in (TWO, 3 * half)],
        scratch_shapes=[pltpu.VMEM(w.shape, BF16) for w in weights] + [pltpu.VMEM((TWO + TWO * half, r, d), BF16)] * TWO + [pltpu.SemaphoreType.DMA] * TWO
        + [pltpu.SemaphoreType.DMA((7,))],
        compiler_params=params(60, collective_id=5 + layer, has_side_effects=True),
        cost_estimate=pl.CostEstimate(flops=10**8, transcendentals=ZERO, bytes_accessed=10**6),
        name="pack",
    )(*weights)


def _meet(*refs, size, n):
    grads, (total_ref, *got), blocks, (part, parts, out_sem, in_sem, swap_out, swap_in, sem) = refs[:n], refs[n : TWO * n + ONE], refs[TWO * n + ONE : 3 * n + ONE], refs[3 * n + ONE :]
    me = lax.axis_index("dp")
    other = dict(device_id={"dp": me + ONE - TWO * lax.rem(me, TWO)}, device_id_type=MESH)
    peer = lambda i: dict(device_id={"dp": lax.rem(me + i, size)}, device_id_type=MESH)
    barrier = pltpu.get_barrier_semaphore()
    for i in range(ONE, size):
        pl.semaphore_signal(barrier, inc=ONE, **peer(i))
    loads = [pltpu.make_async_copy(a, b, sem.at[i]) for i, (a, b) in enumerate(zip(grads, blocks))]
    for c in loads:
        c.start()
    total = jnp.zeros((SUBLANES, LANES), F32)
    for c, ref in zip(loads, blocks):
        c.wait()
        x = ref[...].astype(F32)
        x = jnp.sum(x * x, axis=ZERO)
        x = sum(x[i : i + SUBLANES] for i in range(ZERO, x.shape[ZERO], SUBLANES))
        total += sum(x[:, i : i + LANES] for i in range(ZERO, x.shape[ONE], LANES))
    part[...] = total
    pl.semaphore_wait(barrier, size - ONE)
    swaps = [pltpu.make_async_remote_copy(ref.at[pl.ds(ZERO, to.shape[ZERO])], to, swap_out.at[i], swap_in.at[i], **other)
             for i, (ref, to) in enumerate(zip(blocks, got))]
    for c in swaps:
        c.start()
    sends = [pltpu.make_async_remote_copy(part, parts.at[i], out_sem.at[i], in_sem.at[i], **peer(i)) for i in range(ONE, size)]
    for c in sends:
        c.start()
    parts[ZERO] = part[...]
    for c in sends:
        c.wait()
    total_ref[...] = lax.fori_loop(ZERO, size, lambda j, t: t + parts[lax.rem(me - j + size, size)], jnp.zeros_like(total))
    for c in swaps:
        c.wait()


def meet(grads, shared, size):
    n = len(grads)
    dma = pltpu.SemaphoreType.DMA
    return pl.pallas_call(
        functools.partial(_meet, size=size, n=n),
        in_specs=[IN_HBM] * n,
        out_specs=[IN_VMEM] + [IN_HBM] * n,
        out_shape=[shape((SUBLANES, LANES), F32)] + [shape((k, *x.shape[1:])) for k, x in zip(shared, grads)],
        scratch_shapes=[pltpu.VMEM(x.shape, BF16) for x in grads]
        + [pltpu.VMEM((SUBLANES, LANES), F32), pltpu.VMEM((size, SUBLANES, LANES), F32), dma((size,)), dma((size,)), dma((n,)), dma((n,)), dma((n,))],
        compiler_params=params(60, collective_id=1, has_side_effects=True),
        cost_estimate=pl.CostEstimate(flops=10**9, transcendentals=0, bytes_accessed=10**6),
        name="meet",
    )(*grads)


def _finish(*refs, layers, count, half):
    lists, many = 4 * layers + ONE, 4 * layers + 22
    given, outs, held, (narrow, wide, in_sem, out_sem) = refs[:many], refs[many : many + 21], refs[many + 21 : TWO * many + 21], refs[TWO * many + 21 :]
    loads = [pltpu.make_async_copy(a, b, in_sem.at[i]) for i, (a, b) in enumerate(zip(given, held))]
    for c in loads:
        c.start()
    total_ref, *blocks = held[:lists]
    arrays = held[lists:]
    pairs, inners, other_pairs, other_inners = (blocks[i : i + layers] for i in range(ZERO, 4 * layers, layers))
    r, _, d = arrays[ZERO].shape
    core = lax.rem(lax.axis_index("dp"), TWO)
    for c in loads[:lists]:
        c.wait()
    factor = jnp.minimum(1.0, 0.5 * lax.rsqrt(jnp.full((ONE, ONE), jnp.sum(total_ref[...])) / count + 1e-30))

    def update(j, here, g):
        ws, ms, vs = arrays[j], arrays[7 + j], arrays[14 + j]
        g = g * factor
        m = 0.9 * ms[here] + 0.1 * g
        v = 0.95 * vs[here] + 0.05 * g * g
        w = ws[here].astype(F32)
        ms[here] = m
        vs[here] = v
        ws[here] = (w - 0.02 * (m * lax.rsqrt(v + 1e-8) + 0.1 * w)).astype(BF16)

    def lay(first):
        low, high = ((pairs, inners), (other_pairs, other_inners))[:: ONE if first else -ONE]
        at = slice(ZERO, r) if first else slice(r, TWO * r)
        for n in range(layers):
            for k in range(TWO):
                narrow[k, :, n, :] = low[ZERO][n][k, at].astype(F32)
                narrow[TWO + k, :, n, :] = high[ZERO][n][k, at].astype(F32)
                for i in range(half):
                    wide[k, :, n, i * d : (i + ONE) * d] = low[ONE][n][k * half + i, at].astype(F32)
                    wide[k, :, n, (half + i) * d : (half + i + ONE) * d] = high[ONE][n][k * half + i, at].astype(F32)

    for c in (ZERO, ONE):
        pl.when(core == c)(functools.partial(lay, c == ZERO))
    back = []
    for j in (6, 4, 5, ZERO, ONE, TWO, 3):
        some = range(j, 21, 7)
        for i in some:
            loads[lists + i].wait()
        if j == 6:
            for n in range(layers):
                ref, at = (inners[n], TWO * half) if n == layers - ONE else (pairs[n + ONE], TWO)
                for i in range(half):
                    update(j, (n, slice(i * TWO * r, (i + ONE) * TWO * r)), ref[at + i].astype(F32))
        elif j >= 4:
            for i in range(TWO * half):
                here = (slice(None), slice(None), slice(i * d, (i + ONE) * d))
                update(j, here, wide[(j - 4, *here)])
        else:
            update(j, ..., narrow[j])
        for i in some:
            back.append(pltpu.make_async_copy(arrays[i], outs[i], out_sem.at[i]))
            back[-ONE].start()
    for c in back:
        c.wait()


def finish(total, grads, arrays, count, half):
    layers = len(grads[ZERO])
    given = [total] + [x for some in grads for x in some] + list(arrays)
    outs = [shape(a.shape, a.dtype) for a in arrays]
    r, _, d = arrays[ZERO].shape
    f = arrays[4].shape[TWO]
    dma = pltpu.SemaphoreType.DMA
    return pl.pallas_call(
        functools.partial(_finish, layers=layers, count=count, half=half),
        in_specs=[IN_HBM] * len(given),
        out_specs=[IN_HBM] * len(outs),
        out_shape=outs,
        scratch_shapes=[pltpu.VMEM(x.shape, x.dtype) for x in given]
        + [pltpu.VMEM((4, r, layers, d), F32), pltpu.VMEM((TWO, r, layers, f), F32), dma((len(given),)), dma((len(outs),))],
        compiler_params=params(),
        cost_estimate=cost(10**7, *given, *outs),
        name="finish",
    )(*given)


def rotary(tokens):
    half = HEAD // 2
    angle = np.arange(tokens, dtype=np.float32)[:, None] * np.float32(THETA) ** (-np.arange(half, dtype=np.float32) / np.float32(half))
    cos, sin = np.cos(angle), np.sin(angle)
    return np.concatenate([cos, cos], 1), np.concatenate([-sin, sin], 1)


def solution(mesh):
    size = mesh.shape["dp"]
    chips = size // TWO

    def gathered(blocks):
        k, r, d = blocks.shape
        return lax.all_gather(blocks.reshape(k * r, d), "dp", axis=ZERO, tiled=True).reshape(chips, TWO * k, r, d)

    def scattered(blocks):
        _, k, r, d = blocks.shape
        return lax.psum_scatter(blocks.reshape(-ONE, d), "dp", scatter_dimension=ZERO, tiled=True).reshape(k // TWO, r, d)

    def turn(some):
        return [w.transpose(ONE, ZERO, TWO) for w in some[:6]] + [some[6]]

    def step(x, dy, *arrays):
        weights, m, v = (arrays[i : i + 7] for i in (ZERO, 7, 14))
        layers = weights[ZERO].shape[ZERO]
        h, dy = x[ZERO], dy[ZERO]
        tokens, d = h.shape
        n = weights[4].shape[TWO] // d
        tables = rotary(tokens)

        own, *others = [blocks for i in range(layers) for blocks in pack(turn(weights), n, i)]
        g = [spread(own, size)] + [gathered(blocks) for blocks in others]
        ga, gm = g[::TWO], g[ONE::TWO]
        kept = []
        for i in range(layers):
            q, k, v_ = project(h, ga[i], tables)
            o, lse = attend(q, k, v_)
            kept.append((h, q, k, v_, o, lse))
            if i < layers - ONE:
                h2, b, gate, up, act, h = rest(h, o, ga[i], gm[i], n)
                kept[i] += (h2, b, gate, up, act)
        pairs, inners = [None] * layers, [None] * layers
        half = n // TWO
        for i in reversed(range(layers)):
            h, q, k, v_, o, lse, *more = kept[i]
            end = i == layers - ONE
            if end:
                b, act, dgu, dh, do, delta = rest_last(dy, h, o, ga[i], gm[i], n)
            else:
                h2, b, gate, up, act = more
                dgu, dh, do, delta = rest_back(dy, h2, o, ga[i], gm[i], n, gate, up)
                dgu, inners[i + ONE] = lax.optimization_barrier((dgu, inners[i + ONE]))
            inner, into = weights_back(b, dgu, act, dy, o, dh, gm[i], n, end, 4 + (n if i else ZERO))
            do, inner = lax.optimization_barrier((do, inner))
            inners[i] = scattered(inner)
            if not end:
                do, pairs[i + ONE] = lax.optimization_barrier((do, pairs[i + ONE]))
            dq, dk, dv = attend_back(q, k, v_, do, lse, delta)
            if i:
                dy, into = project_back(h, dh, dq, dk, dv, tables, ga[i], into)
                pairs[i] = scattered(down_back(kept[i - ONE][-ONE], dy, into, n))
            else:
                (into,) = project_back(h, None, dq, dk, dv, tables, ga[i], into)
                pairs[i] = collect(into, size)
        total, *got = meet(pairs + inners, [TWO] * layers + [TWO * half] * layers, size)
        grads = [pairs, inners, got[:layers], got[layers:]]
        done = finish(total, grads, turn(weights) + turn(m) + turn(v), size * sum(w.size for w in weights), half)
        return tuple(t for i in (ZERO, 7, 14) for t in turn(done[i : i + 7]))

    states, cut = P(("rep", "dp"), None, None), P(None, "dp", None)
    return jax.shard_map(
        step,
        mesh=mesh,
        in_specs=(states, states) + (cut,) * 21,
        out_specs=(P("rep", "dp", None),) * 21,
        check_vma=False,
    )
```
